128 devices in a mesh: seq: 32 (over z, x, y_hi), mp: 4 (over y_lo, core).
Axes of the slice: x: 4, y: 4 (y_hi: 2, y_lo: 2; y = y_hi * 2 + y_lo), z: 4, core: 2. Of those that a mesh axis runs over, the one named last changes fastest.
Arguments:
- layer_inputs: bfloat16 [16384, 4096], P('seq', 'mp'), may hold values from -6 to 6
- article_opening: int32 [32], P('seq'), may hold values from 1 to 512, as said below
- blending_ratios: float32 [5, 4096], replicated, may hold values from 0 to 1
- blending_narrow_operand: bfloat16 [4096, 256], P('mp'), may hold values from -0.09375 to 0.09375
- blending_widen_operand: bfloat16 [4, 64, 4096], replicated, may hold values from -0.75 to 0.75
- fading_narrow_operand: bfloat16 [4096, 128], P('mp'), may hold values from -0.09375 to 0.09375
- fading_widen_operand: bfloat16 [128, 2048], P(None, 'mp'), may hold values from -0.5 to 0.5
- fading_anchor: float32 [2048], P('mp'), may hold values from -14 to -3
- immediate_reward: float32 [2048], P('mp'), may hold values from 0.25 to 1.5
- acceptance_weights: bfloat16 [4096, 2048], P(None, 'mp'), may hold values from -0.09375 to 0.09375
- lookup_weights: bfloat16 [4096, 2048], P(None, 'mp'), may hold values from -0.09375 to 0.09375
- payload_weights: bfloat16 [4096, 2048], P(None, 'mp'), may hold values from -0.09375 to 0.09375
- group_scaling_weight: float32 [2048], P('mp'), may hold values from 0.5 to 1.5
- group_scaling_shift: float32 [2048], P('mp'), may hold values from -2 to 2
Outputs:
- time_mix: bfloat16 [16384, 2048], P('seq', 'mp')
The draws below stay inside these ranges and needn't reach their ends.
Inputs may be any that keep to these rules, and one draw needn't show every extreme that they name: `article_opening`: entry j is the offset within shard j of the first token of a document that begins in shard j, or 512 where none begins there; at most one document begins in a shard.
All inputs are finite; a program needn't handle non-finite values.
Results may differ from the reference program's by a relative error of at most 0.0076.
Values may be sent and summed in bfloat16 or wider, within the bound.
No kernel may reach another device: no remote copies, remote signals or barrier semaphores. Data moves between devices by JAX's collectives and lax.ppermute only.
A program may use at most 128 MiB of HBM per device.

```python
import jax
import jax.numpy as jnp
from jax import lax

D = 4096
GROUPS_HERE = 32
GROUP_WIDTH = 64
MIX_RANK = 64
DECAY_RANK = 128
TOK_DEV = 512
TOKENS = 16384
TOTAL_WIDTH = 2048
N_SEQ = 32


def draw_article_opening(key, part):
    pick_key, place_key = jax.random.split(jax.random.fold_in(key, 11))
    shards = TOKENS // TOK_DEV
    chosen = jax.random.randint(pick_key, (shards,), 0, 4)
    offsets = jax.random.randint(place_key, (shards,), 1, TOK_DEV)
    return jnp.where(chosen == 0, offsets, TOK_DEV).astype(jnp.int32)


def draw_fading_anchor(key, part):
    head_key, fast_key, slow_key = jax.random.split(jax.random.fold_in(key, 23), 3)
    fast_share = 0.5
    slow_top = 1.5
    fast_heads = jax.random.bernoulli(head_key, fast_share, (GROUPS_HERE, 1))
    fast_rate = jax.random.uniform(fast_key, (GROUPS_HERE, GROUP_WIDTH), jnp.float32, 1.0 / 50.0, 1.0 / 30.0)
    lowest_log = jnp.log(jnp.float32(0.25) / TOKENS)
    highest_log = jnp.log(jnp.float32(slow_top) / TOK_DEV)
    slow_rate = jnp.exp(jax.random.uniform(slow_key, (GROUPS_HERE, GROUP_WIDTH), jnp.float32, 0.0, 1.0) * (highest_log - lowest_log) + lowest_log)
    rates = jnp.where(fast_heads, fast_rate, slow_rate)
    return jnp.log(rates).reshape(GROUPS_HERE * GROUP_WIDTH).astype(jnp.float32)


def level_of(rng, shape, cuts, low, largest):
    loudness = 1.0
    for dim, parts in cuts:
        draws = jax.random.uniform(jax.random.fold_in(jax.random.fold_in(rng, 6), dim), (parts,), jnp.float32, low / len(cuts), largest / len(cuts))
        loudness = loudness * jnp.repeat(jnp.exp(draws), shape[dim] // parts).reshape((-1,) + (1,) * (len(shape) - 1 - dim))
    return loudness


def gaussian(own_key, extent, deviation, bound, cuts=(), kind=jnp.bfloat16):
    drawn = deviation * jax.random.normal(own_key, extent, jnp.float32)
    if cuts:
        drawn = drawn * level_of(own_key, extent, cuts, -0.22, 0.18)
    return jnp.clip(drawn, -bound, bound).astype(kind)


def setup_inputs(seed: int = 0) -> dict:
    arg_keys = jax.random.split(jax.random.key(seed), 15)
    return {
        "layer_inputs": gaussian(arg_keys[0], (TOKENS, D), 1.0, 6.0, ((0, 32), (1, 4))),
        "article_opening": draw_article_opening(jax.random.fold_in(arg_keys[14], 71), 0),
        "blending_ratios": jnp.clip(jax.random.uniform(arg_keys[2], (5, D), jnp.float32, 0.0, 1.0), 0.0, 1.0),
        "blending_narrow_operand": gaussian(arg_keys[3], (D, 4 * MIX_RANK), D ** -0.5, 0.09375, ((0, 4),)),
        "blending_widen_operand": gaussian(arg_keys[4], (4, MIX_RANK, D), MIX_RANK ** -0.5, 0.75),
        "fading_narrow_operand": gaussian(arg_keys[5], (D, DECAY_RANK), D ** -0.5, 0.09375, ((0, 4),)),
        "fading_widen_operand": gaussian(arg_keys[6], (DECAY_RANK, TOTAL_WIDTH), DECAY_RANK ** -0.5, 0.5, ((1, 4),)),
        "fading_anchor": draw_fading_anchor(jax.random.fold_in(arg_keys[14], 71), 0),
        "immediate_reward": jnp.clip(0.25 + 1.25 * jax.random.uniform(arg_keys[8], (TOTAL_WIDTH,), jnp.float32) ** level_of(arg_keys[8], (TOTAL_WIDTH,), ((0, 4),), -0.2, 0.2), 0.25, 1.5),
        "acceptance_weights": gaussian(arg_keys[9], (D, TOTAL_WIDTH), D ** -0.5, 0.09375, ((1, 4),)),
        "lookup_weights": gaussian(arg_keys[10], (D, TOTAL_WIDTH), D ** -0.5, 0.09375, ((1, 4),)),
        "payload_weights": gaussian(arg_keys[11], (D, TOTAL_WIDTH), D ** -0.5, 0.09375, ((1, 4),)),
        "group_scaling_weight": jnp.clip(1.0 + 0.1 * jax.random.normal(arg_keys[12], (TOTAL_WIDTH,), jnp.float32), 0.5, 1.5),
        "group_scaling_shift": gaussian(arg_keys[13], (TOTAL_WIDTH,), 0.3, 2.0, ((0, 4),), jnp.float32),
    }


def project_rows(rows, before, blending_ratios, blending_narrow_operand, blending_widen_operand, fading_narrow_operand, fading_widen_operand, fading_anchor, acceptance_weights, lookup_weights, payload_weights):
    wide_rows = rows.astype(jnp.float32)
    difference = before.astype(jnp.float32) - wide_rows
    blended = (wide_rows + difference * blending_ratios[0]).astype(jnp.bfloat16)
    rank_hidden = jnp.tanh(jnp.dot(blended, blending_narrow_operand, preferred_element_type=jnp.float32)).astype(jnp.bfloat16)
    mixed_inputs = []
    for branch in range(4):
        delta_rows = jnp.dot(rank_hidden[:, branch * MIX_RANK:(branch + 1) * MIX_RANK], blending_widen_operand[branch], preferred_element_type=jnp.float32)
        mixed_inputs.append((wide_rows + difference * (blending_ratios[branch + 1] + delta_rows)).astype(jnp.bfloat16))
    decay_hidden = jnp.tanh(jnp.dot(mixed_inputs[0], fading_narrow_operand, preferred_element_type=jnp.float32)).astype(jnp.bfloat16)
    log_decay = -jnp.exp(fading_anchor + jnp.dot(decay_hidden, fading_widen_operand, preferred_element_type=jnp.float32))
    acceptance_lines = jnp.dot(mixed_inputs[3], acceptance_weights, preferred_element_type=jnp.float32)
    lookup_mapped = jnp.dot(mixed_inputs[1], lookup_weights, preferred_element_type=jnp.float32)
    value_projected = jnp.dot(mixed_inputs[2], payload_weights, preferred_element_type=jnp.float32)
    return (acceptance_lines, lookup_mapped, value_projected, log_decay)

def reference(layer_inputs, article_opening, blending_ratios, blending_narrow_operand, blending_widen_operand, fading_narrow_operand, fading_widen_operand, fading_anchor, immediate_reward, acceptance_weights, lookup_weights, payload_weights, group_scaling_weight, group_scaling_shift):
    position = jnp.arange(TOKENS, dtype=jnp.int32)
    offset = position % TOK_DEV
    starts = article_opening[position // TOK_DEV]
    unbroken = jnp.logical_and(offset != starts, position > 0)
    previous = jnp.concatenate([jnp.zeros((1, D), jnp.bfloat16), layer_inputs[:-1]], axis=0)
    previous = jnp.where(unbroken[:, None], previous, jnp.zeros_like(previous))

    def per_shard(pair):
        return project_rows(pair[0], pair[1], blending_ratios, blending_narrow_operand, blending_widen_operand, fading_narrow_operand, fading_widen_operand, fading_anchor, acceptance_weights, lookup_weights, payload_weights)
    pieces = lax.map(per_shard, (layer_inputs.reshape(N_SEQ, TOK_DEV, D), previous.reshape(N_SEQ, TOK_DEV, D)))
    acceptance_lines, lookup_mapped, value_projected, log_decay = [piece.reshape(TOKENS, GROUPS_HERE, GROUP_WIDTH) for piece in pieces]
    reward_by_group = immediate_reward.reshape(GROUPS_HERE, GROUP_WIDTH)
    flags = unbroken.astype(jnp.float32)

    def advance(carried, inputs):
        acceptance_latest, lookup_mapped_latest, payload_mapped_latest, decay_now, flag_now = inputs
        retained_state = carried * flag_now
        attention_result = jnp.einsum('je,jez->jz', acceptance_latest, retained_state, precision=lax.Precision.HIGHEST)
        attention_result = attention_result + lax.optimization_barrier(jnp.sum(acceptance_latest * reward_by_group * lookup_mapped_latest, axis=-1))[:, None] * payload_mapped_latest
        carried = jnp.exp(decay_now)[:, :, None] * retained_state + lookup_mapped_latest[:, :, None] * payload_mapped_latest[:, None, :]
        return (carried, attention_result)
    initial = jnp.zeros((GROUPS_HERE, GROUP_WIDTH, GROUP_WIDTH), jnp.float32)
    final_state, outputs = lax.scan(advance, initial, (acceptance_lines, lookup_mapped, value_projected, log_decay, flags))
    centred = outputs - lax.optimization_barrier(jnp.mean(outputs, axis=-1, keepdims=True))
    variance = lax.optimization_barrier(jnp.mean(centred * centred, axis=-1, keepdims=True))
    normed = (centred / jnp.sqrt(variance + 0.00064)).reshape(TOKENS, TOTAL_WIDTH)
    return (normed * group_scaling_weight + group_scaling_shift).astype(jnp.bfloat16)
```

```python
import functools

import jax
import jax.numpy as jnp
import numpy as np
from jax import lax
from jax.experimental import pallas as pl
from jax.experimental.pallas import tpu as pltpu
from jax.sharding import Mesh
from jax.sharding import PartitionSpec as P

F32 = jnp.float32
BF16 = jnp.bfloat16
GROUP = 64
SUB = 64
CHUNK = 128
CTX = 16
HALVES = (32, 16, 8, 4, 2, 1)
FLOOR = -100.0
SEQ = ("z", "x", "y_hi")
MP = ("y_lo", "core")


def xor_permute(array, axes, flip):
    length = lax.axis_size(axes)
    return lax.ppermute(array, axes, [(i, i ^ flip) for i in range(length)])


def dot(a, b):
    return jnp.dot(a, b, preferred_element_type=F32)


def dot_nt(a, b):
    return lax.dot_general(a, b, (((1,), (1,)), ((), ())), preferred_element_type=F32)


def dot_tn(a, b):
    return lax.dot_general(a, b, (((0,), (0,)), ((), ())), preferred_element_type=F32)


def sum_rows():
    t = np.arange(SUB)[:, None]
    j = np.arange(SUB)[None, :]
    blocks = []
    for half in HALVES:
        middle = (t // (2 * half)) * (2 * half) + half - 1
        right = t > middle
        blocks.append(np.where(right, (j > middle) & (j < t), (j > t) & (j <= middle)))
    blocks.append(j < t)
    blocks.append(j > t)
    one = np.concatenate(blocks, 0)
    return np.concatenate([one, one], 1).astype(np.float32)


def project_kernel(where_ref, *refs, first_token):
    mains, ctxs, narrows, fadings = refs[0:4], refs[4:8], refs[8:12], refs[12:16]
    (ratios, widen, w_r, w_k, w_v, fade_widen, anchor, out_r, out_k, out_v, out_w,
     rows, diffs, rank, hidden, mixed, acc) = refs[16:]
    step = pl.program_id(0)
    start = where_ref[1]
    count = rows.shape[1]

    for j in range(4):

        @pl.when(step == j)
        def _(j=j):
            x = mains[j][...].astype(F32)
            line = lax.broadcasted_iota(jnp.int32, x.shape, 0)
            before = pltpu.roll(x, 1, 0)
            before = jnp.where(line == 0, ctxs[j][CTX - 1 : CTX, :].astype(F32), before)
            before = jnp.where(line + first_token == start, 0.0, before)
            d = before - x
            rows[j] = x
            diffs[j] = d
            blended = (x + d * ratios[0:1, :]).astype(BF16)
            part = dot(blended, narrows[j][...])
            if j == 0:
                rank[...] = part
            else:
                rank[...] += part

    @pl.when(step == 4)
    def _():
        total = jnp.tanh(rank[...]).astype(BF16)
        for b in range(4):
            hidden[b] = total[:, 64 * b : 64 * b + 64]

    @pl.when(step >= 4)
    def _():
        j = step - 4
        for b in range(4):
            for n in range(4):
                cols = slice(256 * n, 256 * n + 256)
                delta = dot(hidden[b], widen[b, :, cols])
                mixed[b, :, cols] = (
                    rows[j, :, cols] + diffs[j, :, cols] * (ratios[b + 1 : b + 2, cols] + delta)
                ).astype(BF16)
        for i in range(4):

            @pl.when(j == i)
            def _(i=i):
                part = dot(mixed[0], fadings[i][...])
                if i == 0:
                    acc[...] = part
                else:
                    acc[...] += part

        for b, weights, out in ((1, w_k, out_k), (2, w_v, out_v), (3, w_r, out_r)):
            part = dot(mixed[b], weights[...])

            @pl.when(j == 0)
            def _(part=part, out=out):
                out[...] = part

            @pl.when(j > 0)
            def _(part=part, out=out):
                out[...] += part

    @pl.when(step == 7)
    def _():
        low = jnp.tanh(acc[...]).astype(BF16)
        out_w[...] = -jnp.exp(anchor[...] + dot(low, fade_widen[...]))


def project(where, first_token, mains, ctxs, narrows, fadings, ratios, widen, w_r, w_k, w_v, fade_widen, anchor):
    width = narrows[0].shape[0]
    channels = w_r.shape[1]

    def fixed(shape, index):
        return pl.BlockSpec(shape, lambda s, m: index)

    def late(s, m):
        return m[0] ^ jnp.maximum(s - 4, 0)

    in_specs = [fixed((CHUNK, width), (i, 0)) for _, i in mains]
    in_specs += [fixed((CTX, width), (i, 0)) for _, i in ctxs]
    in_specs += [fixed(a.shape, (0, 0)) for a in narrows + fadings]
    in_specs += [
        pl.BlockSpec((5, width), lambda s, m: (0, m[0] ^ (s % 4))),
        pl.BlockSpec((4, 64, width), lambda s, m: (0, 0, late(s, m))),
        pl.BlockSpec((width, channels), lambda s, m: (late(s, m), 0)),
        pl.BlockSpec((width, channels), lambda s, m: (late(s, m), 0)),
        pl.BlockSpec((width, channels), lambda s, m: (late(s, m), 0)),
        fixed(fade_widen.shape, (0, 0)),
        fixed(anchor.shape, (0, 0)),
    ]
    return pl.pallas_call(
        functools.partial(project_kernel, first_token=first_token),
        grid_spec=pltpu.PrefetchScalarGridSpec(
            num_scalar_prefetch=1,
            grid=(8,),
            in_specs=in_specs,
            out_specs=[fixed((CHUNK, channels), (0, 0))] * 4,
            scratch_shapes=[
                pltpu.VMEM((4, CHUNK, width), F32),
                pltpu.VMEM((4, CHUNK, width), F32),
                pltpu.VMEM((CHUNK, 256), F32),
                pltpu.VMEM((4, CHUNK, 64), BF16),
                pltpu.VMEM((4, CHUNK, width), BF16),
                pltpu.VMEM((CHUNK, 128), F32),
            ],
        ),
        out_shape=[jax.ShapeDtypeStruct((CHUNK, channels), F32)] * 4,
        compiler_params=pltpu.CompilerParams(
            dimension_semantics=("arbitrary",), vmem_limit_bytes=48 * 1024 * 1024
        ),
        cost_estimate=pl.CostEstimate(flops=3 * 10**9, bytes_accessed=17 * 10**6, transcendentals=0),
    )(where, *[a for a, _ in mains], *[a for a, _ in ctxs], *narrows, *fadings, ratios, widen, w_r, w_k, w_v, fade_widen, anchor)


def split_two(w):
    high = w.astype(BF16)
    low = (w - high.astype(F32)).astype(BF16)
    return jnp.concatenate([high, low], 0)


def states_kernel(where_ref, sums, *refs):
    ks, vs, ws = refs[0:4], refs[4:8], refs[8:12]
    entering, whole, packed = refs[12:]
    start = where_ref[1]
    channels = ks[0].shape[1]
    line = lax.broadcasted_iota(jnp.int32, (SUB, 1), 0)
    lane = lax.broadcasted_iota(jnp.int32, (SUB, 128), 1)
    state = jnp.zeros((SUB, channels), F32)
    decay = jnp.ones((1, channels), F32)
    for c in range(8):
        rows = slice(SUB * (c % 2), SUB * (c % 2) + SUB)
        w = jnp.maximum(ws[c // 2][rows, :], FLOOR)
        k = ks[c // 2][rows, :]
        v = vs[c // 2][rows, :].astype(BF16)
        tail = dot(sums[7 * SUB : 8 * SUB, :], split_two(w))
        ends_late = (c * SUB + SUB - 1) >= start
        begins_late = (c * SUB - 1) >= start if c else jnp.bool_(False)
        late = (line + c * SUB) >= start
        keep = late == ends_late
        total = jnp.where(begins_late == ends_late, jnp.exp(tail[0:1, :] + w[0:1, :]), 0.0)
        kk = jnp.where(keep, k * jnp.exp(tail), 0.0).astype(BF16)
        entering[c] = state.astype(BF16)
        pieces = []
        for p in range(channels // 128):
            cols = slice(128 * p, 128 * p + 128)
            both = dot_tn(v[:, cols], kk[:, cols])
            pieces.append(jnp.where(lane < GROUP, both[0:GROUP], both[GROUP:128]))
        state = state * total + jnp.concatenate(pieces, 1)
        decay = decay * total
    whole[0:SUB, :] = state
    whole[SUB : SUB + 8, :] = jnp.broadcast_to(decay, (8, channels))
    packed[0:SUB, :] = state.astype(BF16)
    high = decay.astype(BF16)
    low = (decay - high.astype(F32)).astype(BF16)
    packed[SUB : SUB + 8, :] = jnp.broadcast_to(high, (8, channels))
    packed[SUB + 8 : SUB + 16, :] = jnp.broadcast_to(low, (8, channels))


SMEM = pl.BlockSpec(memory_space=pltpu.SMEM)
VMEM = pl.BlockSpec(memory_space=pltpu.VMEM)


def shard_states(where, sums, ks, vs, ws):
    channels = ks[0].shape[1]
    return pl.pallas_call(
        states_kernel,
        in_specs=[SMEM] + [VMEM] * 13,
        out_specs=[VMEM] * 3,
        out_shape=[
            jax.ShapeDtypeStruct((8, SUB, channels), BF16),
            jax.ShapeDtypeStruct((SUB + 8, channels), F32),
            jax.ShapeDtypeStruct((SUB + 16, channels), BF16),
        ],
        compiler_params=pltpu.CompilerParams(vmem_limit_bytes=32 * 1024 * 1024),
        cost_estimate=pl.CostEstimate(flops=10**9, bytes_accessed=4 * 10**6, transcendentals=0),
    )(where, sums, *ks, *vs, *ws)


def local_kernel(where_ref, sums, reward, entering, *refs):
    rs, ks, vs, ws = refs[0:4], refs[4:8], refs[8:12], refs[12:16]
    local, queries = refs[16:]
    start = where_ref[1]
    channels = rs[0].shape[1]
    line = lax.broadcasted_iota(jnp.int32, (SUB, 1), 0)
    lane = lax.broadcasted_iota(jnp.int32, (SUB, 128), 1)
    two_t = lax.broadcasted_iota(jnp.int32, (2 * SUB, SUB), 0) % SUB
    two_s = lax.broadcasted_iota(jnp.int32, (2 * SUB, SUB), 1)
    before = jnp.zeros((1, channels), F32)

    def apart(a):
        zero = jnp.zeros_like(a)
        return jnp.concatenate([jnp.where(lane < GROUP, a, zero), jnp.where(lane < GROUP, zero, a)], 0)

    for c in range(8):
        rows = slice(SUB * (c % 2), SUB * (c % 2) + SUB)
        w = jnp.maximum(ws[c // 2][rows, :], FLOOR)
        r = rs[c // 2][rows, :]
        k = ks[c // 2][rows, :]
        v = vs[c // 2][rows, :].astype(BF16)
        sides = []
        exponents = dot(sums[0 : 7 * SUB, :], split_two(w))
        for level, half in enumerate(HALVES):
            right = (line // half) % 2 == 1
            e = jnp.exp(exponents[SUB * level : SUB * level + SUB, :])
            sides.append((jnp.where(right, r, k) * e).astype(BF16))
        before_here = exponents[6 * SUB : 7 * SUB, :]
        late = (line + c * SUB) >= start
        begins_late = (c * SUB - 1) >= start if c else jnp.bool_(False)
        reach = jnp.where(late == begins_late, r * jnp.exp(before_here), 0.0).astype(BF16)
        queries[SUB * c : SUB * c + SUB, :] = jnp.where(late, 0.0, r * jnp.exp(before + before_here)).astype(BF16)
        before = before + before_here[SUB - 1 : SUB, :] + w[SUB - 1 : SUB, :]
        own = (r * reward[...]).astype(BF16)
        k_own = k.astype(BF16)
        same = ((two_t + c * SUB) >= start) == ((two_s + c * SUB) >= start)
        for p in range(channels // 128):
            cols = slice(128 * p, 128 * p + 128)
            scores = jnp.where(two_t == two_s, dot_nt(apart(own[:, cols]), k_own[:, cols]), 0.0)
            for level, half in enumerate(HALVES):
                side = sides[level][:, cols]
                part = dot_nt(apart(side), side)
                here = (two_t // (2 * half) == two_s // (2 * half)) & ((two_t // half) % 2 == 1) & ((two_s // half) % 2 == 0)
                scores = jnp.where(here & same, part, scores)
            both = dot(scores.astype(BF16), v[:, cols])
            out = jnp.where(lane < GROUP, both[0:SUB], both[SUB : 2 * SUB])
            out = out + dot_nt(reach[:, cols], apart(entering[c, :, cols]))
            local[SUB * c : SUB * c + SUB, cols] = out


def local_outputs(where, sums, reward, entering, rs, ks, vs, ws):
    channels = ks[0].shape[1]
    tokens = CHUNK * len(ks)
    return pl.pallas_call(
        local_kernel,
        in_specs=[SMEM] + [VMEM] * 19,
        out_specs=[VMEM] * 2,
        out_shape=[
            jax.ShapeDtypeStruct((tokens, channels), F32),
            jax.ShapeDtypeStruct((tokens, channels), BF16),
        ],
        compiler_params=pltpu.CompilerParams(vmem_limit_bytes=40 * 1024 * 1024),
        cost_estimate=pl.CostEstimate(flops=6 * 10**9, bytes_accessed=6 * 10**6, transcendentals=0),
    )(where, sums, reward, entering, *rs, *ks, *vs, *ws)


def finish_kernel(local, queries, incoming, gain, shift, out):
    channels = local.shape[1]
    lane = lax.broadcasted_iota(jnp.int32, (SUB, 128), 1)
    row = lax.broadcasted_iota(jnp.int32, (128, 128), 0)
    col = lax.broadcasted_iota(jnp.int32, (128, 128), 1)
    average = jnp.where((row // GROUP) == (col // GROUP), 1.0 / GROUP, 0.0).astype(BF16)
    for p in range(channels // 128):
        cols = slice(128 * p, 128 * p + 128)
        st = incoming[:, cols].astype(BF16)
        zero = jnp.zeros_like(st)
        st = jnp.concatenate([jnp.where(lane < GROUP, st, zero), jnp.where(lane < GROUP, zero, st)], 0)
        o = local[:, cols] + dot_nt(queries[:, cols], st)
        high = o.astype(BF16)
        low = (o - high.astype(F32)).astype(BF16)
        centred = o - (dot(high, average) + dot(low, average))
        square = centred * centred
        high = square.astype(BF16)
        low = (square - high.astype(F32)).astype(BF16)
        variance = dot(high, average) + dot(low, average)
        normed = centred * lax.rsqrt(variance + 0.00064)
        out[:, cols] = (normed * gain[:, cols] + shift[:, cols]).astype(BF16)


def finish(local, queries, incoming, gain, shift):
    return pl.pallas_call(
        finish_kernel,
        in_specs=[VMEM] * 5,
        out_specs=VMEM,
        out_shape=jax.ShapeDtypeStruct(local.shape, BF16),
        compiler_params=pltpu.CompilerParams(vmem_limit_bytes=32 * 1024 * 1024),
        cost_estimate=pl.CostEstimate(flops=10**9, bytes_accessed=2 * 10**6, transcendentals=0),
    )(local, queries, incoming, gain, shift)


def unpack(packed):
    decay = packed[SUB : SUB + 1].astype(F32) + packed[SUB + 8 : SUB + 9].astype(F32)
    return decay, packed[0:SUB].astype(F32)


def pack(decay, state):
    high = decay.astype(BF16)
    low = (decay - high.astype(F32)).astype(BF16)
    wide = (8, decay.shape[1])
    return jnp.concatenate([state.astype(BF16), jnp.broadcast_to(high, wide), jnp.broadcast_to(low, wide)], 0)


def combine(earlier, later):
    return earlier[0] * later[0], later[0] * earlier[1] + later[1]


def choose(flag, a, b):
    return jax.tree.map(lambda u, v: jnp.where(flag, u, v), a, b)


def incoming_state(whole, packed):
    own = (whole[SUB : SUB + 1], whole[0:SUB])
    start = (jnp.ones_like(own[0]), jnp.zeros_like(own[1]))
    before = start
    for axis in reversed(SEQ):
        length, here = lax.axis_size(axis), lax.axis_index(axis)
        pieces = [own] + [unpack(xor_permute(packed, axis, k)) for k in range(1, length)]
        inside, so_far = start, start
        for m in range(length):
            from_m = pieces[m]
            for other in range(1, length):
                from_m = choose(here == other, pieces[m ^ other], from_m)
            inside = choose(m == here, so_far, inside)
            so_far = combine(so_far, from_m)
        before = combine(inside, before)
        own = so_far
        packed = pack(*own)
    return before[1]


def body(
    layer_inputs,
    article_opening,
    blending_ratios,
    blending_narrow_operand,
    blending_widen_operand,
    fading_narrow_operand,
    fading_widen_operand,
    fading_anchor,
    immediate_reward,
    acceptance_weights,
    lookup_weights,
    payload_weights,
    group_scaling_weight,
    group_scaling_shift,
):
    x = layer_inputs
    channels = fading_anchor.shape[0]
    where = jnp.stack([lax.axis_index(MP).astype(jnp.int32), article_opening[0]])
    shards = lax.axis_size(SEQ)

    def across_far(a):
        return lax.ppermute(a, ("y_hi", "y_lo"), [(i, i ^ 3) for i in range(4)])

    def partner(a):
        return xor_permute(a, MP, 1)

    def across(a):
        return xor_permute(a, MP, 2)

    part = [x[128 * c : 128 * c + 128] for c in range(4)]
    before = lax.ppermute(x[-CTX:], SEQ, [(i, i + 1) for i in range(shards - 1)])
    far_a = across(jnp.concatenate([part[1], x[128 - CTX : 128]], 0))
    far_narrow = across_far(blending_narrow_operand)
    near = partner(x)
    far_b = across(part[2])
    far_c = across(part[3])
    far_d = across(jnp.concatenate([part[0], before], 0))
    far_fading = across_far(fading_narrow_operand)
    narrows = [blending_narrow_operand, partner(blending_narrow_operand), far_narrow, partner(far_narrow)]
    fadings = [fading_narrow_operand, partner(fading_narrow_operand), far_fading, partner(far_fading)]
    near_before = partner(before)
    far = [far_d, far_a, far_b, far_c]
    cross = [partner(f) for f in far]
    done = [None] * 4
    for c in (1, 2, 3, 0):
        mains = [(x, c), (near, c), (far[c], 0), (cross[c], 0)]
        if c == 0:
            ctxs = [(before, 0), (near_before, 0), (far[0], 8), (cross[0], 8)]
        elif c == 1:
            ctxs = [(x, 7), (near, 7), (far[1], 8), (cross[1], 8)]
        else:
            ctxs = [(x, 8 * c - 1), (near, 8 * c - 1), (far[c - 1], 7), (cross[c - 1], 7)]
        done[c] = project(
            where, CHUNK * c, mains, ctxs, narrows, fadings, blending_ratios, blending_widen_operand,
            acceptance_weights, lookup_weights, payload_weights, fading_widen_operand, fading_anchor[None],
        )
    rs, ks, vs, ws = zip(*done)
    sums = jnp.asarray(sum_rows(), BF16)
    entering, whole, packed = shard_states(where, sums, ks, vs, ws)
    local, queries = local_outputs(where, sums, immediate_reward[None], entering, rs, ks, vs, ws)
    incoming = incoming_state(whole, packed)
    return finish(local, queries, incoming, group_scaling_weight[None], group_scaling_shift[None])


def solution(mesh):
    torus = Mesh(mesh.devices.reshape(4, 4, 2, 2, 2), ("z", "x", "y_hi", "y_lo", "core"))
    placed = (
        P(SEQ, MP),
        P(SEQ),
        P(),
        P(MP, None),
        P(),
        P(MP, None),
        P(None, MP),
        P(MP),
        P(MP),
        P(None, MP),
        P(None, MP),
        P(None, MP),
        P(MP),
        P(MP),
    )
    return jax.shard_map(body, mesh=torus, in_specs=placed, out_specs=P(SEQ, MP), check_vma=False)
```

```python
import functools

import jax
import jax.numpy as jnp
import numpy as np
from jax import lax
from jax.experimental import pallas as pl
from jax.experimental.pallas import tpu as pltpu
from jax.sharding import Mesh
from jax.sharding import PartitionSpec as P


F32 = jnp.float32
BF16 = jnp.bfloat16
GROUP = 64
SUB = 64
LAST = 192
SPLIT = 160
CTX = 16
HALVES = (32, 16, 8, 4, 2, 1)
FLOOR = -100.0
SEQ = ("z", "x", "y_hi")
MP = ("y_lo", "core")


def xor_permute(array, axes, flip):
    length = lax.axis_size(axes)
    return lax.ppermute(array, axes, [(i, i ^ flip) for i in range(length)])


def dot(a, b):
    return jnp.dot(a, b, preferred_element_type=F32)


def dot_nt(a, b):
    return lax.dot_general(a, b, (((1,), (1,)), ((), ())), preferred_element_type=F32)


def dot_tn(a, b):
    return lax.dot_general(a, b, (((0,), (0,)), ((), ())), preferred_element_type=F32)


def sum_rows():
    t = np.arange(SUB)[:, None]
    j = np.arange(SUB)[None, :]
    blocks = []
    for half in HALVES:
        middle = (t // (2 * half)) * (2 * half) + half - 1
        right = t > middle
        blocks.append(np.where(right, (j > middle) & (j < t), (j > t) & (j <= middle)))
    blocks.append(j < t)
    blocks.append(j > t)
    one = np.concatenate(blocks, 0)
    return np.concatenate([one, one], 1).astype(np.float32)


SMEM = pl.BlockSpec(memory_space=pltpu.SMEM)
VMEM = pl.BlockSpec(memory_space=pltpu.VMEM)


def in_hbm(array):
    return pltpu.with_memory_space_constraint(array, pltpu.HBM)


def in_vmem(array):
    return pltpu.with_memory_space_constraint(array, pltpu.VMEM)


def load_kernel(where_ref, widen_far, w_r_far, w_k_far, w_v_far, *refs):
    count = (len(refs) - 5) // 2
    small_far, (widen, w_r, w_k, w_v), small, ready = refs[:count], refs[count : count + 4], refs[count + 4 : -1], refs[-1]
    width = w_r.shape[1]
    copies = [pltpu.make_async_copy(a, b, ready.at[4, i]) for i, (a, b) in enumerate(zip(small_far, small))]
    for j in range(4):
        there = pl.ds(pl.multiple_of((where_ref[0] ^ j) * width, width), width)
        copies.append(pltpu.make_async_copy(widen_far.at[:, :, there], widen.at[j], ready.at[j, 0]))
        for i, source, target in ((1, w_k_far, w_k), (2, w_v_far, w_v), (3, w_r_far, w_r)):
            copies.append(pltpu.make_async_copy(source.at[there, :], target.at[j], ready.at[j, i]))
    for copy in copies:
        copy.start()
    for copy in copies:
        copy.wait()


def load(where, widen, w_r, w_k, w_v, *small):
    channels = w_r.shape[1]
    width = w_r.shape[0] // 4
    return pl.pallas_call(
        load_kernel,
        in_specs=[SMEM] + [pl.BlockSpec(memory_space=pltpu.HBM)] * (4 + len(small)),
        out_specs=[VMEM] * (4 + len(small)),
        scratch_shapes=[pltpu.SemaphoreType.DMA((5, max(4, len(small))))],
        out_shape=[pltpu.VMEM((4, 4, 64, width), BF16)]
        + [pltpu.VMEM((4, width, channels), BF16)] * 3
        + [pltpu.VMEM(a.shape, a.dtype) for a in small],
        compiler_params=pltpu.CompilerParams(vmem_limit_bytes=2**20),
        cost_estimate=pl.CostEstimate(flops=5 * 10**9, bytes_accessed=15 * 10**6, transcendentals=0),
    )(where, *map(in_hbm, (widen, w_r, w_k, w_v, *small)))


def read_rows(refs, cols):
    parts = [ref[:, cols] for ref in refs]
    return parts[0] if len(parts) == 1 else jnp.concatenate(parts, 0)


def project_rows(me, start, first_token, pieces, narrows, fadings, weights, out, scratch):
    ratios, fade_widen, anchor, widen, w_r, w_k, w_v = weights
    diffs, mixed_a, mixed_b = scratch
    tokens, width = diffs.shape[1:]
    channels = w_r.shape[2]
    tile = 256
    line = lax.broadcasted_iota(jnp.int32, (tokens, tile), 0)
    first = line == 0
    opens = line + first_token == start

    rank = jnp.zeros((tokens, 256), F32)
    for j in range(4):
        base = (me ^ j) * width
        parts = []
        for n in range(width // tile):
            cols = slice(tile * n, tile * n + tile)
            rows = read_rows(pieces[j], cols).astype(F32)
            x = rows[CTX:]
            before = jnp.where(first, rows[CTX - 1 : CTX], pltpu.roll(x, 1, 0))
            d = jnp.where(opens, 0.0, before) - x
            diffs[j, :, cols] = d
            ratio = ratios[0:1, pl.ds(pl.multiple_of(base + tile * n, tile), tile)]
            parts.append((x + d * ratio).astype(BF16))
        rank = rank + dot(jnp.concatenate(parts, 1), narrows[j][...])
    total = jnp.tanh(rank).astype(BF16)
    hidden = [total[:, 64 * b : 64 * b + 64] for b in range(4)]

    def mix(j, mixed):
        base = (me ^ j) * width
        for n in range(width // tile):
            cols = slice(tile * n, tile * n + tile)
            there = pl.ds(pl.multiple_of(base + tile * n, tile), tile)
            x = read_rows(pieces[j], cols)[CTX:].astype(F32)
            d = diffs[j, :, cols]
            for b in range(4):
                delta = dot(hidden[b], widen[j, b, :, cols])
                mixed[b, :, cols] = (x + d * (ratios[b + 1 : b + 2, there] + delta)).astype(BF16)

    def project_piece(j, mixed, low):
        low = low + dot(mixed[0], fadings[j][...])
        for b, w, at in ((1, w_k, 1), (2, w_v, 2), (3, w_r, 0)):
            part = dot(mixed[b], w[j])
            cols = slice(channels * at, channels * at + channels)
            if j == 0:
                out[:, cols] = part
            else:
                out[:, cols] += part
        return low

    slots = (mixed_a, mixed_b)
    low = jnp.zeros((tokens, 128), F32)
    mix(0, slots[0])
    for j in range(4):
        if j < 3:
            mix(j + 1, slots[(j + 1) % 2])
        low = project_piece(j, slots[j % 2], low)
    low = jnp.tanh(low).astype(BF16)
    out[:, 3 * channels :] = -jnp.exp(anchor[...] + dot(low, fade_widen[...]))


def take_pieces(refs, counts):
    pieces = []
    for count in counts:
        pieces.append(refs[:count])
        refs = refs[count:]
    return pieces, refs


def late_kernel(where_ref, *refs, first_token, counts):
    pieces, refs = take_pieces(refs, counts)
    project_rows(where_ref[0], where_ref[1], first_token, pieces, refs[0:4], refs[4:8], refs[8:15], refs[15], refs[16:])


def early_kernel(where_ref, *refs, counts):
    pieces, refs = take_pieces(refs, counts)
    sums, late, out, entering, offsets, whole, packed = refs[15:22]
    project_rows(where_ref[0], where_ref[1], 0, pieces, refs[0:4], refs[4:8], refs[8:15], out, refs[22:])
    states(where_ref[1], sums, (out, late), entering, offsets, whole, packed)


def project_scratch(tokens, width):
    return [pltpu.VMEM((4, tokens, width), F32)] + [pltpu.VMEM((4, tokens, width), BF16)] * 2


def project_late(where, pieces, narrows, fadings, weights, tokens):
    width, channels = narrows[0].shape[0], weights[4].shape[2]
    counts = tuple(len(p) for p in pieces)
    operands = [a for p in pieces for a in p] + [*narrows, *fadings, *weights]
    return pl.pallas_call(
        functools.partial(late_kernel, first_token=LAST, counts=counts),
        in_specs=[SMEM] + [VMEM] * len(operands),
        out_specs=VMEM,
        scratch_shapes=project_scratch(tokens, width),
        out_shape=pltpu.VMEM((tokens, 4 * channels), F32),
        compiler_params=pltpu.CompilerParams(vmem_limit_bytes=(2 * 1024 + 48 * tokens) * 1024),
        cost_estimate=pl.CostEstimate(flops=25 * 10**6 * tokens, bytes_accessed=17 * 10**6, transcendentals=0),
    )(where, *operands[: -len(weights)], *map(in_vmem, weights))


def project_early(where, pieces, narrows, fadings, weights, sums, late):
    width, channels = narrows[0].shape[0], weights[4].shape[2]
    counts = tuple(len(p) for p in pieces)
    operands = [a for p in pieces for a in p] + [*narrows, *fadings, *weights, sums, late]
    return pl.pallas_call(
        functools.partial(early_kernel, counts=counts),
        in_specs=[SMEM] + [VMEM] * len(operands),
        out_specs=[VMEM] * 5,
        scratch_shapes=project_scratch(LAST, width),
        out_shape=[
            pltpu.VMEM((LAST, 4 * channels), F32),
            pltpu.VMEM((8, SUB, channels), BF16),
            pltpu.VMEM((8, channels), F32),
            jax.ShapeDtypeStruct((SUB + 8, channels), F32),
            jax.ShapeDtypeStruct((SUB + 16, channels), BF16),
        ],
        compiler_params=pltpu.CompilerParams(vmem_limit_bytes=(2 * 1024 + 48 * LAST) * 1024),
        cost_estimate=pl.CostEstimate(flops=25 * 10**6 * LAST, bytes_accessed=17 * 10**6, transcendentals=0),
    )(where, *operands[: -2 - len(weights)], *map(in_vmem, operands[-2 - len(weights) :]))


def split_two(w):
    high = w.astype(BF16)
    low = (w - high.astype(F32)).astype(BF16)
    return jnp.concatenate([high, low], 0)


def sub_chunk(chunks, c, channels):
    ref, at = (chunks[0], SUB * c) if SUB * c < LAST else (chunks[1], SUB * c - LAST)
    r, k, v, w = [ref[at : at + SUB, channels * i : channels * i + channels] for i in range(4)]
    return r, k, v.astype(BF16), jnp.maximum(w, FLOOR)


def states(start, sums, chunks, entering, offsets, whole, packed):
    channels = entering.shape[2]
    line = lax.broadcasted_iota(jnp.int32, (SUB, 1), 0)
    lane = lax.broadcasted_iota(jnp.int32, (SUB, 128), 1)
    state = jnp.zeros((SUB, channels), F32)
    decay = jnp.ones((1, channels), F32)
    offset = jnp.zeros((1, channels), F32)
    for c in range(8):
        _, k, v, w = sub_chunk(chunks, c, channels)
        tail = dot(sums[7 * SUB : 8 * SUB, :], split_two(w))
        ends_late = (c * SUB + SUB - 1) >= start
        begins_late = (c * SUB - 1) >= start if c else jnp.bool_(False)
        late = (line + c * SUB) >= start
        keep = late == ends_late
        log_total = tail[0:1, :] + w[0:1, :]
        total = jnp.where(begins_late == ends_late, jnp.exp(log_total), 0.0)
        offsets[c : c + 1, :] = offset
        offset = offset + log_total
        kk = jnp.where(keep, k * jnp.exp(tail), 0.0).astype(BF16)
        entering[c] = state.astype(BF16)
        pieces = []
        for p in range(channels // 128):
            cols = slice(128 * p, 128 * p + 128)
            both = dot_tn(v[:, cols], kk[:, cols])
            pieces.append(jnp.where(lane < GROUP, both[0:GROUP], both[GROUP:128]))
        state = state * total + jnp.concatenate(pieces, 1)
        decay = decay * total
    whole[0:SUB, :] = state
    whole[SUB : SUB + 8, :] = jnp.broadcast_to(decay, (8, channels))
    packed[0:SUB, :] = state.astype(BF16)
    high = decay.astype(BF16)
    low = (decay - high.astype(F32)).astype(BF16)
    packed[SUB : SUB + 8, :] = jnp.broadcast_to(high, (8, channels))
    packed[SUB + 8 : SUB + 16, :] = jnp.broadcast_to(low, (8, channels))


def local_kernel(where_ref, sums, reward, entering, offsets, chunk, local, queries, *, numbers, first_token):
    start = where_ref[1]
    channels = local.shape[1]
    line = lax.broadcasted_iota(jnp.int32, (SUB, 1), 0)
    lane = lax.broadcasted_iota(jnp.int32, (SUB, 128), 1)
    two_t = lax.broadcasted_iota(jnp.int32, (2 * SUB, SUB), 0) % SUB
    two_s = lax.broadcasted_iota(jnp.int32, (2 * SUB, SUB), 1)

    def apart(a):
        zero = jnp.zeros_like(a)
        return jnp.concatenate([jnp.where(lane < GROUP, a, zero), jnp.where(lane < GROUP, zero, a)], 0)

    for n, c in enumerate(numbers):
        at = SUB * c - first_token
        r, k, v, w = [chunk[at : at + SUB, channels * i : channels * i + channels] for i in range(4)]
        v = v.astype(BF16)
        w = jnp.maximum(w, FLOOR)
        sides = []
        exponents = dot(sums[0 : 7 * SUB, :], split_two(w))
        for level, half in enumerate(HALVES):
            right = (line // half) % 2 == 1
            e = jnp.exp(exponents[SUB * level : SUB * level + SUB, :])
            sides.append((jnp.where(right, r, k) * e).astype(BF16))
        before_here = exponents[6 * SUB : 7 * SUB, :]
        late = (line + c * SUB) >= start
        begins_late = (c * SUB - 1) >= start if c else jnp.bool_(False)
        reach = jnp.where(late == begins_late, r * jnp.exp(before_here), 0.0).astype(BF16)
        offset = offsets[c : c + 1, :]
        rows = slice(SUB * n, SUB * n + SUB)
        queries[rows, :] = jnp.where(late, 0.0, r * jnp.exp(offset + before_here)).astype(BF16)
        own = (r * reward[...]).astype(BF16)
        k_own = k.astype(BF16)
        same = ((two_t + c * SUB) >= start) == ((two_s + c * SUB) >= start)
        for p in range(channels // 128):
            cols = slice(128 * p, 128 * p + 128)
            scores = jnp.where(two_t == two_s, dot_nt(apart(own[:, cols]), k_own[:, cols]), 0.0)
            for level, half in enumerate(HALVES):
                side = sides[level][:, cols]
                part = dot_nt(apart(side), side)
                here = (two_t // (2 * half) == two_s // (2 * half)) & ((two_t // half) % 2 == 1) & ((two_s // half) % 2 == 0)
                scores = jnp.where(here & same, part, scores)
            both = dot(scores.astype(BF16), v[:, cols])
            out = jnp.where(lane < GROUP, both[0:SUB], both[SUB : 2 * SUB])
            local[rows, cols] = out + dot_nt(reach[:, cols], apart(entering[c, :, cols]))


def local_outputs(where, sums, reward, entering, offsets, chunk, numbers, first_token):
    channels = entering.shape[2]
    tokens = len(numbers) * SUB
    return pl.pallas_call(
        functools.partial(local_kernel, numbers=numbers, first_token=first_token),
        in_specs=[SMEM] + [VMEM] * 5,
        out_specs=[VMEM] * 2,
        out_shape=[pltpu.VMEM((tokens, channels), F32), pltpu.VMEM((tokens, channels), BF16)],
        compiler_params=pltpu.CompilerParams(vmem_limit_bytes=6 * 1024 * 1024),
        cost_estimate=pl.CostEstimate(flops=2 * 10**9, bytes_accessed=3 * 10**6, transcendentals=0),
    )(where, *map(in_vmem, (sums, reward, entering, offsets, chunk)))


def unpack(ref):
    return ref[SUB : SUB + 1].astype(F32) + ref[SUB + 8 : SUB + 9].astype(F32), ref[0:SUB].astype(F32)


def pack(ref, decay, state):
    high = decay.astype(BF16)
    low = (decay - high.astype(F32)).astype(BF16)
    wide = (8, decay.shape[1])
    ref[0:SUB, :] = state.astype(BF16)
    ref[SUB : SUB + 8, :] = jnp.broadcast_to(high, wide)
    ref[SUB + 8 : SUB + 16, :] = jnp.broadcast_to(low, wide)


def store(ref, decay, state):
    ref[0:SUB, :] = state
    ref[SUB : SUB + 8, :] = jnp.broadcast_to(decay, (8, decay.shape[1]))


def combine(earlier, later):
    return earlier[0] * later[0], later[0] * earlier[1] + later[1]


def choose(flag, a, b):
    return tuple(jnp.where(flag, u, v) for u, v in zip(a, b))


def along_axis(here, own, received, before):
    pieces = [own] + [unpack(ref) for ref in received]
    length = len(pieces)
    start = (jnp.ones_like(own[0]), jnp.zeros_like(own[1]))
    inside, so_far = start, None
    for m in range(length):
        from_m = pieces[m]
        for other in range(1, length):
            from_m = choose(here == other, pieces[m ^ other], from_m)
        if m:
            inside = choose(here == m, so_far, inside)
        so_far = from_m if so_far is None else combine(so_far, from_m)
    return inside if before is None else combine(inside, before), so_far


def merge_kernel(where_ref, *refs, place, count, opening):
    whole, refs = refs[0], refs[1:]
    before = None
    if not opening:
        before, refs = (refs[0][SUB : SUB + 1], refs[0][0:SUB]), refs[1:]
    received, (whole_out, packed_out, before_out) = refs[:count], refs[count:]
    own = (whole[SUB : SUB + 1], whole[0:SUB])
    before, total = along_axis(where_ref[place], own, received, before)
    store(whole_out, *total)
    pack(packed_out, *total)
    store(before_out, *before)


def merge(where, place, whole, before, received):
    channels = whole.shape[1]
    operands = [whole] + ([] if before is None else [before]) + received
    return pl.pallas_call(
        functools.partial(merge_kernel, place=place, count=len(received), opening=before is None),
        in_specs=[SMEM] + [VMEM] * len(operands),
        out_specs=[VMEM] * 3,
        out_shape=[
            jax.ShapeDtypeStruct((SUB + 8, channels), F32),
            jax.ShapeDtypeStruct((SUB + 16, channels), BF16),
            jax.ShapeDtypeStruct((SUB + 8, channels), F32),
        ],
        compiler_params=pltpu.CompilerParams(vmem_limit_bytes=4 * 1024 * 1024),
        cost_estimate=pl.CostEstimate(flops=10**8, bytes_accessed=10**6, transcendentals=0),
    )(where, *operands)


def finish_kernel(where_ref, *refs, parts, place):
    locals_, queries, refs = refs[:parts], refs[parts : 2 * parts], refs[2 * parts :]
    gain, shift, whole, before, *received, out, held, ready = refs
    own = (whole[SUB : SUB + 1], whole[0:SUB])
    (_, incoming), _ = along_axis(where_ref[place], own, received, (before[SUB : SUB + 1], before[0:SUB]))
    incoming = incoming.astype(BF16)
    channels = gain.shape[1]
    lane = lax.broadcasted_iota(jnp.int32, (SUB, 128), 1)
    row = lax.broadcasted_iota(jnp.int32, (128, 128), 0)
    col = lax.broadcasted_iota(jnp.int32, (128, 128), 1)
    average = jnp.where((row // GROUP) == (col // GROUP), 1.0 / GROUP, 0.0).astype(BF16)
    copies = []
    at = 0
    for i in range(parts):
        rows = slice(at, at + locals_[i].shape[0])
        at = rows.stop
        for p in range(channels // 128):
            cols = slice(128 * p, 128 * p + 128)
            st = incoming[:, cols]
            zero = jnp.zeros_like(st)
            st = jnp.concatenate([jnp.where(lane < GROUP, st, zero), jnp.where(lane < GROUP, zero, st)], 0)
            o = locals_[i][:, cols] + dot_nt(queries[i][:, cols], st)
            high = o.astype(BF16)
            low = (o - high.astype(F32)).astype(BF16)
            centred = o - (dot(high, average) + dot(low, average))
            square = centred * centred
            high = square.astype(BF16)
            low = (square - high.astype(F32)).astype(BF16)
            variance = dot(high, average) + dot(low, average)
            normed = centred * lax.rsqrt(variance + 0.00064)
            held[rows, cols] = (normed * gain[:, cols] + shift[:, cols]).astype(BF16)
        copies.append(pltpu.make_async_copy(held.at[rows, :], out.at[rows, :], ready.at[i]))
        copies[-1].start()
    for copy in copies:
        copy.wait()


def finish(where, place, locals_, queries, gain, shift, whole, before, received):
    parts = len(locals_)
    tokens, channels = sum(a.shape[0] for a in locals_), gain.shape[1]
    return pl.pallas_call(
        functools.partial(finish_kernel, parts=parts, place=place),
        in_specs=[SMEM] + [VMEM] * (2 * parts + 4 + len(received)),
        out_specs=pl.BlockSpec(memory_space=pltpu.HBM),
        scratch_shapes=[pltpu.VMEM((tokens, channels), BF16), pltpu.SemaphoreType.DMA((parts,))],
        out_shape=jax.ShapeDtypeStruct((tokens, channels), BF16),
        compiler_params=pltpu.CompilerParams(vmem_limit_bytes=6 * 1024 * 1024),
        cost_estimate=pl.CostEstimate(flops=10**9, bytes_accessed=2 * 10**6, transcendentals=0),
    )(where, *map(in_vmem, (*locals_, *queries, gain, shift)), whole, before, *received)


def inner(
    layer_inputs,
    article_opening,
    blending_ratios,
    blending_narrow_operand,
    blending_widen_operand,
    fading_narrow_operand,
    fading_widen_operand,
    fading_anchor,
    immediate_reward,
    acceptance_weights,
    lookup_weights,
    payload_weights,
    group_scaling_weight,
    group_scaling_shift,
):
    x = layer_inputs
    places = [lax.axis_index(axis).astype(jnp.int32) for axis in (MP, *SEQ)]
    where = jnp.stack([places[0], article_opening[0], *places[1:]])
    shards = lax.axis_size(SEQ)

    def across_far(a):
        return lax.ppermute(a, ("y_hi", "y_lo"), [(i, i ^ 3) for i in range(4)])

    def partner(a):
        return xor_permute(a, MP, 1)

    def across(a):
        return xor_permute(a, MP, 2)

    late_rows = x.shape[0] - LAST
    cut = LAST + SPLIT
    own_late = [x[LAST - CTX : cut], x[cut:]]
    far_late_a = across(own_late[0])
    far_narrow = across_far(blending_narrow_operand)
    near_narrow = partner(blending_narrow_operand)
    near_late_a = partner(own_late[0])
    before = lax.ppermute(x[-CTX:], SEQ, [(i, i + 1) for i in range(shards - 1)])
    far_late_b = across(own_late[1])
    near_late_b = partner(own_late[1])
    far_fading = across_far(fading_narrow_operand)
    near_fading = partner(fading_narrow_operand)
    own_early = jnp.concatenate([before, x[:LAST]], 0)
    far_early = across(own_early)
    near_early = partner(own_early)
    next_late_a = partner(far_late_a)
    next_narrow = partner(far_narrow)
    next_late_b = partner(far_late_b)
    next_fading = partner(far_fading)
    sums = jnp.asarray(sum_rows(), BF16)
    (widen, w_r, w_k, w_v, narrow, fading, ratios, fade_widen, anchor, sums, reward, gain, shift) = load(
        where, blending_widen_operand, acceptance_weights, lookup_weights, payload_weights,
        blending_narrow_operand, fading_narrow_operand, blending_ratios, fading_widen_operand, fading_anchor[None],
        sums, immediate_reward[None], group_scaling_weight[None], group_scaling_shift[None],
    )
    narrows = [narrow, near_narrow, far_narrow, next_narrow]
    fadings = [fading, near_fading, far_fading, next_fading]
    weights = (ratios, fade_widen, anchor, widen, w_r, w_k, w_v)
    pieces = [own_late, [near_late_a, near_late_b], [far_late_a, far_late_b], [next_late_a, next_late_b]]
    late = project_late(where, pieces, narrows, fadings, weights, late_rows)
    far_early, late = lax.optimization_barrier((far_early, late))
    next_early = partner(far_early)
    pieces = [[own_early], [near_early], [far_early], [next_early]]
    early, entering, offsets, whole, packed = project_early(where, pieces, narrows, fadings, weights, sums, late)
    outputs = []
    for chunk, numbers, first_token in ((early, (0, 1, 2), 0), (late, (3, 4), LAST), (late, (5, 6, 7), LAST)):
        outputs.append(local_outputs(where, sums, reward, entering, offsets, chunk, numbers, first_token))
    before = None
    for axis in reversed(SEQ):
        received = []
        for k in range(1, lax.axis_size(axis)):
            received.append(xor_permute(packed, axis, k))
        place = 2 + SEQ.index(axis)
        if axis != SEQ[0]:
            whole, packed, before = merge(where, place, whole, before, received)
    locals_, queries = zip(*outputs)
    return finish(where, place, locals_, queries, gain, shift, whole, before, received)


def solution(mesh):
    torus = Mesh(mesh.devices.reshape(4, 4, 2, 2, 2), ("z", "x", "y_hi", "y_lo", "core"))
    placed = (
        P(SEQ, MP),
        P(SEQ),
        P(),
        P(MP, None),
        P(),
        P(MP, None),
        P(None, MP),
        P(MP),
        P(MP),
        P(None, MP),
        P(None, MP),
        P(None, MP),
        P(MP),
        P(MP),
    )
    return jax.shard_map(inner, mesh=torus, in_specs=placed, out_specs=P(SEQ, MP), check_vma=False)
```

```python
import functools

import jax
import jax.numpy as jnp
import numpy as np
from jax import lax
from jax.experimental import pallas as pl
from jax.experimental.pallas import tpu as pltpu
from jax.sharding import Mesh
from jax.sharding import PartitionSpec as P


F32 = jnp.float32
BF16 = jnp.bfloat16
GROUP = 64
SUB = 64
LAST = 256
SPLIT = 128
CTX = 16
HALVES = (32, 16, 8, 4, 2, 1)
FLOOR = -100.0
SEQ = ("z", "x", "y_hi")
MP = ("y_lo", "core")


def xor_permute(array, axes, flip):
    length = lax.axis_size(axes)
    return lax.ppermute(array, axes, [(i, i ^ flip) for i in range(length)])


def dot(a, b):
    return jnp.dot(a, b, preferred_element_type=F32)


def dot_nt(a, b):
    return lax.dot_general(a, b, (((1,), (1,)), ((), ())), preferred_element_type=F32)


def dot_tn(a, b):
    return lax.dot_general(a, b, (((0,), (0,)), ((), ())), preferred_element_type=F32)


def sum_rows():
    t = np.arange(SUB)[:, None]
    j = np.arange(SUB)[None, :]
    blocks = []
    for half in HALVES:
        middle = (t // (2 * half)) * (2 * half) + half - 1
        right = t > middle
        blocks.append(np.where(right, (j > middle) & (j < t), (j > t) & (j <= middle)))
    blocks.append(j < t)
    blocks.append(j > t)
    one = np.concatenate(blocks, 0)
    return np.concatenate([one, one], 1).astype(np.float32)


SMEM = pl.BlockSpec(memory_space=pltpu.SMEM)
VMEM = pl.BlockSpec(memory_space=pltpu.VMEM)


def in_hbm(array):
    return pltpu.with_memory_space_constraint(array, pltpu.HBM)


def in_vmem(array):
    return pltpu.with_memory_space_constraint(array, pltpu.VMEM)


def cut_kernel(where_ref, x, late_a, late_b, early, last, ready):
    tokens = x.shape[0]
    moves = (
        (x.at[LAST - CTX : LAST + SPLIT, :], late_a),
        (x.at[tokens - CTX :, :], last),
        (x.at[LAST + SPLIT :, :], late_b),
        (x.at[0:LAST, :], early.at[CTX:, :]),
    )
    copies = [pltpu.make_async_copy(a, b, ready.at[i]) for i, (a, b) in enumerate(moves)]
    for copy in copies:
        copy.start()
    early[0:CTX, :] = jnp.zeros((CTX, early.shape[1]), BF16)
    for copy in copies:
        copy.wait()


def cut(where, x):
    tokens, width = x.shape
    return pl.pallas_call(
        cut_kernel,
        in_specs=[SMEM, pl.BlockSpec(memory_space=pltpu.HBM)],
        out_specs=[VMEM] * 4,
        scratch_shapes=[pltpu.SemaphoreType.DMA((4,))],
        out_shape=[
            pltpu.VMEM((CTX + SPLIT, width), BF16),
            pltpu.VMEM((tokens - LAST - SPLIT, width), BF16),
            pltpu.VMEM((CTX + LAST, width), BF16),
            pltpu.VMEM((CTX, width), BF16),
        ],
        compiler_params=pltpu.CompilerParams(vmem_limit_bytes=2**20),
        cost_estimate=pl.CostEstimate(flops=10**6, bytes_accessed=2 * 10**6, transcendentals=0),
    )(where, in_hbm(x))


def load_kernel(where_ref, *refs, kinds):
    count = len(kinds)
    ready = refs[2 * count]
    copies = []
    for i, kind in enumerate(kinds):
        source, target = refs[i], refs[count + i]
        if kind == "plain":
            copies.append(pltpu.make_async_copy(source, target, ready.at[i, 0]))
            continue
        width = target.shape[-1] if kind == "lanes" else target.shape[1]
        for j in range(4):
            there = pl.ds(pl.multiple_of((where_ref[0] ^ j) * width, width), width)
            block = source.at[:, :, there] if kind == "lanes" else source.at[there, :]
            copies.append(pltpu.make_async_copy(block, target.at[j], ready.at[i, j]))
    for copy in copies:
        copy.start()
    for copy in copies:
        copy.wait()


def load(where, *jobs):
    kinds, arrays = zip(*jobs)
    shapes = []
    for kind, a in jobs:
        if kind == "rows":
            shapes.append((4, a.shape[0] // 4, a.shape[1]))
        elif kind == "lanes":
            shapes.append((4, *a.shape[:2], a.shape[2] // 4))
        else:
            shapes.append(a.shape)
    return pl.pallas_call(
        functools.partial(load_kernel, kinds=kinds),
        in_specs=[SMEM] + [pl.BlockSpec(memory_space=pltpu.HBM)] * len(jobs),
        out_specs=[VMEM] * len(jobs),
        scratch_shapes=[pltpu.SemaphoreType.DMA((len(jobs), 4))],
        out_shape=[pltpu.VMEM(shape, a.dtype) for shape, a in zip(shapes, arrays)],
        compiler_params=pltpu.CompilerParams(vmem_limit_bytes=2**20),
        cost_estimate=pl.CostEstimate(flops=3 * 10**9, bytes_accessed=8 * 10**6, transcendentals=0),
    )(where, *map(in_hbm, arrays))


def read_rows(refs, cols):
    parts = [ref[:, cols] for ref in refs]
    return parts[0] if len(parts) == 1 else jnp.concatenate(parts, 0)


def mix_rows(me, start, first_token, pieces, narrows, weights, diffs, slots, consume, branches=(0, 1, 2, 3)):
    ratios, widen = weights
    tokens, width = diffs.shape[1:]
    tile = 256
    line = lax.broadcasted_iota(jnp.int32, (tokens, tile), 0)
    first = line == 0
    opens = line + first_token == start

    rank = jnp.zeros((tokens, 256), F32)
    for j in range(4):
        base = (me ^ j) * width
        parts = []
        for n in range(width // tile):
            cols = slice(tile * n, tile * n + tile)
            rows = read_rows(pieces[j], cols).astype(F32)
            x = rows[CTX:]
            before = jnp.where(first, rows[CTX - 1 : CTX], pltpu.roll(x, 1, 0))
            d = jnp.where(opens, 0.0, before) - x
            diffs[j, :, cols] = d
            ratio = ratios[0:1, pl.ds(pl.multiple_of(base + tile * n, tile), tile)]
            parts.append((x + d * ratio).astype(BF16))
        rank = rank + dot(jnp.concatenate(parts, 1), narrows[j][...])
    total = jnp.tanh(rank).astype(BF16)
    hidden = [total[:, 64 * b : 64 * b + 64] for b in range(4)]

    def mix(j):
        base = (me ^ j) * width
        for n in range(width // tile):
            cols = slice(tile * n, tile * n + tile)
            there = pl.ds(pl.multiple_of(base + tile * n, tile), tile)
            x = read_rows(pieces[j], cols)[CTX:].astype(F32)
            d = diffs[j, :, cols]
            for b in branches:
                delta = dot(hidden[b], widen[j, b, :, cols])
                slots(j, b)[:, cols] = (x + d * (ratios[b + 1 : b + 2, there] + delta)).astype(BF16)

    mix(0)
    for j in range(4):
        if j < 3:
            mix(j + 1)
        consume(j)
    return hidden


def add_product(out, cols, j, rows, weights):
    part = dot(rows[...], weights[j])
    if j == 0:
        out[:, cols] = part
    else:
        out[:, cols] += part


def decay_of(low, fade_widen, anchor):
    return -jnp.exp(anchor[...] + dot(jnp.tanh(low).astype(BF16), fade_widen[...]))


def take_pieces(refs, counts):
    pieces = []
    for count in counts:
        pieces.append(refs[:count])
        refs = refs[count:]
    return pieces, refs


def late_kernel(where_ref, *refs, counts):
    pieces, refs = take_pieces(refs, counts)
    narrows, refs = refs[0:4], refs[4:]
    ratios, widen, w_k, w_v_far, w_r_far, pair, recept, fading_rows, w_v, w_r, diffs, mixed, ready = refs
    channels, width = recept.shape[1], w_k.shape[1]

    def fetch(j, i):
        there = pl.ds(pl.multiple_of((where_ref[0] ^ j) * width, width), width)
        source, target = ((w_v_far, w_v), (w_r_far, w_r))[i]
        return pltpu.make_async_copy(source.at[there, :], target.at[j], ready.at[j, i])

    for j in range(4):
        for i in range(2):
            fetch(j, i).start()

    def slots(j, b):
        return fading_rows.at[j] if b == 0 else mixed.at[j % 2, b - 1]

    def consume(j):
        add_product(pair, slice(0, channels), j, slots(j, 1), w_k)
        fetch(j, 0).wait()
        add_product(pair, slice(channels, 2 * channels), j, slots(j, 2), w_v)
        fetch(j, 1).wait()
        add_product(recept, slice(None), j, slots(j, 3), w_r)

    mix_rows(where_ref[0], where_ref[1], LAST, pieces, narrows, (ratios, widen), diffs, slots, consume)


def decay_kernel(where_ref, rows, *refs):
    fadings, (fade_widen, anchor, sums, pair, out, partial, reach, whole) = refs[0:4], refs[4:]
    tokens, _ = out.shape
    low = dot(rows[0], fadings[0][...])
    for j in range(1, 4):
        low = low + dot(rows[j], fadings[j][...])
    out[...] = decay_of(low, fade_widen, anchor)
    count = tokens // SUB

    def note(n, state, decay, offset):
        partial[n] = state
        reach[n : n + 1, :] = decay
        reach[count + n : count + n + 1, :] = offset

    numbers = range(LAST // SUB, LAST // SUB + count)
    state, decay, _ = add_states(where_ref[1], sums, pair, out, numbers, LAST, note)
    store(whole, decay, state)


def early_kernel(where_ref, *refs, counts):
    pieces, refs = take_pieces(refs, counts)
    narrows, fadings, refs = refs[0:4], refs[4:8], refs[8:]
    ratios, widen, w_k, w_v, fade_widen, anchor, sums, partial, reach, late_whole = refs[:10]
    pair, decay, entering, offsets, whole, packed, diffs, hidden, mixed = refs[10:]
    channels = decay.shape[1]
    low = [None]

    def slots(j, b):
        return mixed.at[j % 2, b]

    def consume(j):
        part = dot(slots(j, 0)[...], fadings[j][...])
        low[0] = part if j == 0 else low[0] + part
        add_product(pair, slice(0, channels), j, slots(j, 1), w_k)
        add_product(pair, slice(channels, 2 * channels), j, slots(j, 2), w_v)

    ranks = mix_rows(
        where_ref[0], where_ref[1], 0, pieces, narrows, (ratios, widen), diffs, slots, consume, branches=(0, 1, 2)
    )
    hidden[...] = ranks[3]
    decay[...] = decay_of(low[0], fade_widen, anchor)

    def note(n, state, _, offset):
        entering[n] = state.astype(BF16)
        offsets[n : n + 1, :] = offset

    count, more = LAST // SUB, partial.shape[0]
    state, total, offset = add_states(where_ref[1], sums, pair, decay, range(count), 0, note)
    final = combine((total, state), (late_whole[SUB : SUB + 1], late_whole[0:SUB]))
    store(whole, *final)
    pack(packed, *final)
    for n in range(more):
        entering[count + n] = (partial[n] + reach[n : n + 1, :] * state).astype(BF16)
        offsets[count + n : count + n + 1, :] = offset + reach[more + n : more + n + 1, :]


def recept_kernel(where_ref, *refs, counts):
    pieces, refs = take_pieces(refs, counts)
    diffs, hidden, ratios, widen, w_r, out, mixed = refs
    width = diffs.shape[2]
    tile = 256
    for j in range(4):
        base = (where_ref[0] ^ j) * width
        for n in range(width // tile):
            cols = slice(tile * n, tile * n + tile)
            there = pl.ds(pl.multiple_of(base + tile * n, tile), tile)
            x = read_rows(pieces[j], cols)[CTX:].astype(F32)
            delta = dot(hidden[...], widen[j, 3, :, cols])
            mixed[j, :, cols] = (x + diffs[j, :, cols] * (ratios[4:5, there] + delta)).astype(BF16)
        add_product(out, slice(None), j, mixed.at[j], w_r)


def recept_early(where, pieces, diffs, hidden, ratios, widen, w_r):
    tokens, width = diffs.shape[1:]
    counts = tuple(len(p) for p in pieces)
    operands = [a for p in pieces for a in p]
    return pl.pallas_call(
        functools.partial(recept_kernel, counts=counts),
        in_specs=[SMEM] + [VMEM] * (len(operands) + 5),
        out_specs=VMEM,
        scratch_shapes=[pltpu.VMEM((4, tokens, width), BF16)],
        out_shape=pltpu.VMEM((tokens, w_r.shape[2]), F32),
        compiler_params=pltpu.CompilerParams(vmem_limit_bytes=7 * 2**20),
        cost_estimate=pl.CostEstimate(flops=2 * 10**9, bytes_accessed=5 * 10**6, transcendentals=0),
    )(where, *operands, *map(in_vmem, (diffs, hidden, ratios, widen, w_r)))


def project_late(where, pieces, narrows, ratios, widen, w_k, w_v, w_r):
    width, channels = w_k.shape[1:]
    counts = tuple(len(p) for p in pieces)
    tokens = sum(a.shape[0] for a in pieces[0]) - CTX
    operands = [a for p in pieces for a in p] + narrows
    return pl.pallas_call(
        functools.partial(late_kernel, counts=counts),
        in_specs=[SMEM] + [VMEM] * (len(operands) + 3) + [pl.BlockSpec(memory_space=pltpu.HBM)] * 2,
        out_specs=[VMEM] * 5,
        scratch_shapes=[
            pltpu.VMEM((4, tokens, width), F32),
            pltpu.VMEM((2, 3, tokens, width), BF16),
            pltpu.SemaphoreType.DMA((4, 2)),
        ],
        out_shape=[
            pltpu.VMEM((tokens, 2 * channels), F32),
            pltpu.VMEM((tokens, channels), F32),
            pltpu.VMEM((4, tokens, width), BF16),
            pltpu.VMEM((4, width, channels), BF16),
            pltpu.VMEM((4, width, channels), BF16),
        ],
        compiler_params=pltpu.CompilerParams(vmem_limit_bytes=(4 * 1024 + 40 * tokens) * 1024),
        cost_estimate=pl.CostEstimate(flops=25 * 10**6 * tokens, bytes_accessed=17 * 10**6, transcendentals=0),
    )(where, *operands, *map(in_vmem, (ratios, widen, w_k)), in_hbm(w_v), in_hbm(w_r))


def decay_late(where, rows, fadings, fade_widen, anchor, sums, pair):
    tokens, channels = rows.shape[1], anchor.shape[1]
    count = tokens // SUB
    return pl.pallas_call(
        decay_kernel,
        in_specs=[SMEM] + [VMEM] * 9,
        out_specs=[VMEM] * 4,
        out_shape=[
            pltpu.VMEM((tokens, channels), F32),
            pltpu.VMEM((count, SUB, channels), F32),
            pltpu.VMEM((2 * count, channels), F32),
            pltpu.VMEM((SUB + 8, channels), F32),
        ],
        compiler_params=pltpu.CompilerParams(vmem_limit_bytes=5 * 2**20),
        cost_estimate=pl.CostEstimate(flops=10**9, bytes_accessed=2 * 10**6, transcendentals=0),
    )(where, in_vmem(rows), *fadings, *map(in_vmem, (fade_widen, anchor, sums, pair)))


def project_early(where, pieces, narrows, fadings, weights, *rest):
    width, channels = weights[2].shape[1:]
    counts = tuple(len(p) for p in pieces)
    operands = [a for p in pieces for a in p] + narrows + fadings
    return pl.pallas_call(
        functools.partial(early_kernel, counts=counts),
        in_specs=[SMEM] + [VMEM] * (len(operands) + len(weights) + len(rest)),
        out_specs=[VMEM] * 8,
        scratch_shapes=[pltpu.VMEM((2, 3, LAST, width), BF16)],
        out_shape=[
            pltpu.VMEM((LAST, 2 * channels), F32),
            pltpu.VMEM((LAST, channels), F32),
            pltpu.VMEM((8, SUB, channels), BF16),
            pltpu.VMEM((8, channels), F32),
            jax.ShapeDtypeStruct((SUB + 8, channels), F32),
            jax.ShapeDtypeStruct((SUB + 8, channels), BF16),
            pltpu.VMEM((4, LAST, width), F32),
            pltpu.VMEM((LAST, 64), BF16),
        ],
        compiler_params=pltpu.CompilerParams(vmem_limit_bytes=(5 * 1024 + 16 * LAST) * 1024),
        cost_estimate=pl.CostEstimate(flops=25 * 10**6 * LAST, bytes_accessed=17 * 10**6, transcendentals=0),
    )(where, *operands, *map(in_vmem, (*weights, *rest)))


def split_two(w):
    high = w.astype(BF16)
    low = (w - high.astype(F32)).astype(BF16)
    return jnp.concatenate([high, low], 0)


def add_states(start, sums, pair, decays, numbers, first_token, note):
    channels = decays.shape[1]
    line = lax.broadcasted_iota(jnp.int32, (SUB, 1), 0)
    lane = lax.broadcasted_iota(jnp.int32, (SUB, 128), 1)
    state = jnp.zeros((SUB, channels), F32)
    decay = jnp.ones((1, channels), F32)
    offset = jnp.zeros((1, channels), F32)
    for n, c in enumerate(numbers):
        note(n, state, decay, offset)
        at = SUB * c - first_token
        w = jnp.maximum(decays[at : at + SUB, :], FLOOR)
        k = pair[at : at + SUB, 0:channels]
        v = pair[at : at + SUB, channels : 2 * channels].astype(BF16)
        tail = dot(sums[7 * SUB : 8 * SUB, :], split_two(w))
        ends_late = (c * SUB + SUB - 1) >= start
        begins_late = (c * SUB - 1) >= start if c else jnp.bool_(False)
        late = (line + c * SUB) >= start
        log_total = tail[0:1, :] + w[0:1, :]
        total = jnp.where(begins_late == ends_late, jnp.exp(log_total), 0.0)
        kk = jnp.where(late == ends_late, k * jnp.exp(tail), 0.0).astype(BF16)
        pieces = []
        for p in range(channels // 128):
            cols = slice(128 * p, 128 * p + 128)
            both = dot_tn(v[:, cols], kk[:, cols])
            pieces.append(jnp.where(lane < GROUP, both[0:GROUP], both[GROUP:128]))
        state = state * total + jnp.concatenate(pieces, 1)
        decay = decay * total
        offset = offset + log_total
    return state, decay, offset


def local_kernel(where_ref, sums, reward, entering, offsets, recept, pair, decay, local, queries, *, first, count, first_token):
    start = where_ref[1]
    channels = local.shape[1]
    line = lax.broadcasted_iota(jnp.int32, (SUB, 1), 0)
    lane = lax.broadcasted_iota(jnp.int32, (SUB, 128), 1)
    two_t = lax.broadcasted_iota(jnp.int32, (2 * SUB, SUB), 0) % SUB
    two_s = lax.broadcasted_iota(jnp.int32, (2 * SUB, SUB), 1)

    def apart(a):
        zero = jnp.zeros_like(a)
        return jnp.concatenate([jnp.where(lane < GROUP, a, zero), jnp.where(lane < GROUP, zero, a)], 0)

    for n in range(count):
        c = first + n
        at = SUB * c - first_token
        there = slice(at, at + SUB)
        r = recept[there, :]
        k, v = [pair[there, channels * i : channels * i + channels] for i in range(2)]
        w = decay[there, :]
        v = v.astype(BF16)
        w = jnp.maximum(w, FLOOR)
        sides = []
        exponents = dot(sums[0 : 7 * SUB, :], split_two(w))
        for level, half in enumerate(HALVES):
            right = (line // half) % 2 == 1
            e = jnp.exp(exponents[SUB * level : SUB * level + SUB, :])
            sides.append((jnp.where(right, r, k) * e).astype(BF16))
        before_here = exponents[6 * SUB : 7 * SUB, :]
        late = (line + c * SUB) >= start
        begins_late = (c * SUB - 1) >= start if c else jnp.bool_(False)
        reach = jnp.where(late == begins_late, r * jnp.exp(before_here), 0.0).astype(BF16)
        offset = offsets[c : c + 1, :]
        rows = slice(SUB * n, SUB * n + SUB)
        queries[rows, :] = jnp.where(late, 0.0, r * jnp.exp(offset + before_here)).astype(BF16)
        own = (r * reward[...]).astype(BF16)
        k_own = k.astype(BF16)
        same = ((two_t + c * SUB) >= start) == ((two_s + c * SUB) >= start)
        for p in range(channels // 128):
            cols = slice(128 * p, 128 * p + 128)
            scores = jnp.where(two_t == two_s, dot_nt(apart(own[:, cols]), k_own[:, cols]), 0.0)
            for level, half in enumerate(HALVES):
                side = sides[level][:, cols]
                part = dot_nt(apart(side), side)
                here = (two_t // (2 * half) == two_s // (2 * half)) & ((two_t // half) % 2 == 1) & ((two_s // half) % 2 == 0)
                scores = jnp.where(here & same, part, scores)
            both = dot(scores.astype(BF16), v[:, cols])
            out = jnp.where(lane < GROUP, both[0:SUB], both[SUB : 2 * SUB])
            local[rows, cols] = out + dot_nt(reach[:, cols], apart(entering[c, :, cols]))


def local_outputs(where, sums, reward, entering, offsets, recept, pair, decay, numbers, first_token):
    channels = entering.shape[2]
    tokens = len(numbers) * SUB
    return pl.pallas_call(
        functools.partial(local_kernel, first=numbers[0], count=len(numbers), first_token=first_token),
        in_specs=[SMEM] + [VMEM] * 7,
        out_specs=[VMEM] * 2,
        out_shape=[pltpu.VMEM((tokens, channels), F32), pltpu.VMEM((tokens, channels), BF16)],
        compiler_params=pltpu.CompilerParams(vmem_limit_bytes=8 * 1024 * 1024),
        cost_estimate=pl.CostEstimate(flops=2 * 10**9, bytes_accessed=3 * 10**6, transcendentals=0),
    )(where, *map(in_vmem, (sums, reward, entering, offsets, recept, pair, decay)))


def unpack(ref):
    return ref[SUB : SUB + 1].astype(F32) + ref[SUB + 1 : SUB + 2].astype(F32), ref[0:SUB].astype(F32)


def pack(ref, decay, state):
    high = decay.astype(BF16)
    low = (decay - high.astype(F32)).astype(BF16)
    wide = (8, decay.shape[1])
    line = lax.broadcasted_iota(jnp.int32, wide, 0)
    high, low = high.astype(F32), low.astype(F32)
    ref[0:SUB, :] = state.astype(BF16)
    ref[SUB : SUB + 8, :] = jnp.where(line == 0, high, jnp.where(line == 1, low, 0.0)).astype(BF16)


def store(ref, decay, state):
    ref[0:SUB, :] = state
    ref[SUB : SUB + 8, :] = jnp.broadcast_to(decay, (8, decay.shape[1]))


def combine(earlier, later):
    return earlier[0] * later[0], later[0] * earlier[1] + later[1]


def choose(flag, a, b):
    return tuple(jnp.where(flag, u, v) for u, v in zip(a, b))


def along_axis(here, own, received, before):
    pieces = [own] + [unpack(ref) for ref in received]
    length = len(pieces)
    start = (jnp.ones_like(own[0]), jnp.zeros_like(own[1]))
    inside, so_far = start, None
    for m in range(length):
        from_m = pieces[m]
        for other in range(1, length):
            from_m = choose(here == other, pieces[m ^ other], from_m)
        if m:
            inside = choose(here == m, so_far, inside)
        so_far = from_m if so_far is None else combine(so_far, from_m)
    return inside if before is None else combine(inside, before), so_far


def merge_kernel(where_ref, *refs, place, count, opening):
    whole, refs = refs[0], refs[1:]
    before = None
    if not opening:
        before, refs = (refs[0][SUB : SUB + 1], refs[0][0:SUB]), refs[1:]
    received, (whole_out, packed_out, before_out) = refs[:count], refs[count:]
    own = (whole[SUB : SUB + 1], whole[0:SUB])
    before, total = along_axis(where_ref[place], own, received, before)
    store(whole_out, *total)
    pack(packed_out, *total)
    store(before_out, *before)


def merge(where, place, whole, before, received):
    channels = whole.shape[1]
    operands = [whole] + ([] if before is None else [before]) + received
    return pl.pallas_call(
        functools.partial(merge_kernel, place=place, count=len(received), opening=before is None),
        in_specs=[SMEM] + [VMEM] * len(operands),
        out_specs=[VMEM] * 3,
        out_shape=[
            jax.ShapeDtypeStruct((SUB + 8, channels), F32),
            jax.ShapeDtypeStruct((SUB + 8, channels), BF16),
            jax.ShapeDtypeStruct((SUB + 8, channels), F32),
        ],
        compiler_params=pltpu.CompilerParams(vmem_limit_bytes=4 * 1024 * 1024),
        cost_estimate=pl.CostEstimate(flops=10**8, bytes_accessed=10**6, transcendentals=0),
    )(where, *operands)


def finish_kernel(where_ref, *refs, parts, place):
    locals_, queries, refs = refs[:parts], refs[parts : 2 * parts], refs[2 * parts :]
    gain, shift, whole, before, *received, out, held, ready = refs
    own = (whole[SUB : SUB + 1], whole[0:SUB])
    (_, incoming), _ = along_axis(where_ref[place], own, received, (before[SUB : SUB + 1], before[0:SUB]))
    incoming = incoming.astype(BF16)
    channels = gain.shape[1]
    lane = lax.broadcasted_iota(jnp.int32, (SUB, 128), 1)
    row = lax.broadcasted_iota(jnp.int32, (128, 128), 0)
    col = lax.broadcasted_iota(jnp.int32, (128, 128), 1)
    average = jnp.where((row // GROUP) == (col // GROUP), 1.0 / GROUP, 0.0).astype(BF16)
    copies = []
    at = 0
    for i in range(parts):
        rows = slice(at, at + locals_[i].shape[0])
        at = rows.stop
        for p in range(channels // 128):
            cols = slice(128 * p, 128 * p + 128)
            st = incoming[:, cols]
            zero = jnp.zeros_like(st)
            st = jnp.concatenate([jnp.where(lane < GROUP, st, zero), jnp.where(lane < GROUP, zero, st)], 0)
            o = locals_[i][:, cols] + dot_nt(queries[i][:, cols], st)
            centred = o - dot(o.astype(BF16), average)
            variance = dot((centred * centred).astype(BF16), average)
            normed = centred * lax.rsqrt(variance + 0.00064)
            held[rows, cols] = (normed * gain[:, cols] + shift[:, cols]).astype(BF16)
        copies.append(pltpu.make_async_copy(held.at[rows, :], out.at[rows, :], ready.at[i]))
        copies[-1].start()
    for copy in copies:
        copy.wait()


def finish(where, place, locals_, queries, gain, shift, whole, before, received):
    parts = len(locals_)
    tokens, channels = sum(a.shape[0] for a in locals_), gain.shape[1]
    return pl.pallas_call(
        functools.partial(finish_kernel, parts=parts, place=place),
        in_specs=[SMEM] + [VMEM] * (2 * parts + 4 + len(received)),
        out_specs=pl.BlockSpec(memory_space=pltpu.HBM),
        scratch_shapes=[pltpu.VMEM((tokens, channels), BF16), pltpu.SemaphoreType.DMA((parts,))],
        out_shape=jax.ShapeDtypeStruct((tokens, channels), BF16),
        compiler_params=pltpu.CompilerParams(vmem_limit_bytes=8 * 1024 * 1024),
        cost_estimate=pl.CostEstimate(flops=10**9, bytes_accessed=2 * 10**6, transcendentals=0),
    )(where, *map(in_vmem, (*locals_, *queries, gain, shift)), whole, before, *received)


def inner(
    layer_inputs,
    article_opening,
    blending_ratios,
    blending_narrow_operand,
    blending_widen_operand,
    fading_narrow_operand,
    fading_widen_operand,
    fading_anchor,
    immediate_reward,
    acceptance_weights,
    lookup_weights,
    payload_weights,
    group_scaling_weight,
    group_scaling_shift,
):
    x = layer_inputs
    places = [lax.axis_index(axis).astype(jnp.int32) for axis in (MP, *SEQ)]
    where = jnp.stack([places[0], article_opening[0], *places[1:]])
    shards = lax.axis_size(SEQ)

    def across_far(a):
        return lax.ppermute(a, ("y_hi", "y_lo"), [(i, i ^ 3) for i in range(4)])

    def partner(a):
        return xor_permute(a, MP, 1)

    def across(a):
        return xor_permute(a, MP, 2)

    late_a, late_b, own_early, last = cut(where, x)
    own_late = [late_a, late_b]
    far_late_a = across(late_a)
    far_narrow = across_far(blending_narrow_operand)
    near_narrow = partner(blending_narrow_operand)
    far_fading = across_far(fading_narrow_operand)
    near_fading = partner(fading_narrow_operand)
    near_late_a = partner(late_a)
    before = lax.ppermute(last, SEQ, [(i, i + 1) for i in range(shards - 1)])
    far_late_b = across(late_b)
    near_late_b = partner(late_b)
    own_early = lax.dynamic_update_slice(own_early, before, (0, 0))
    far_early = across(own_early)
    near_early = partner(own_early)
    sums = jnp.asarray(sum_rows(), BF16)
    widen, w_k, ratios, narrow, fade_widen, anchor, sums, reward, gain, shift, fading = load(
        where, ("lanes", blending_widen_operand), ("rows", lookup_weights), ("plain", blending_ratios),
        ("plain", blending_narrow_operand), ("plain", fading_widen_operand), ("plain", fading_anchor[None]),
        ("plain", sums), ("plain", immediate_reward[None]), ("plain", group_scaling_weight[None]),
        ("plain", group_scaling_shift[None]), ("plain", fading_narrow_operand),
    )
    next_late_a = partner(far_late_a)
    next_narrow = partner(far_narrow)
    next_fading = partner(far_fading)
    next_late_b = partner(far_late_b)
    narrows = [narrow, near_narrow, far_narrow, next_narrow]
    fadings = [fading, near_fading, far_fading, next_fading]
    pieces = [own_late, [near_late_a, near_late_b], [far_late_a, far_late_b], [next_late_a, next_late_b]]
    late, late_recept, fading_rows, w_v, w_r = project_late(
        where, pieces, narrows, ratios, widen, w_k, payload_weights, acceptance_weights
    )
    far_early, late = lax.optimization_barrier((far_early, late))
    late_decay, partial, reach, late_whole = decay_late(where, fading_rows, fadings, fade_widen, anchor, sums, late)
    next_early = partner(far_early)
    pieces = [[own_early], [near_early], [far_early], [next_early]]
    early, decay, entering, offsets, whole, packed, diffs, hidden = project_early(
        where, pieces, narrows, fadings, (ratios, widen, w_k, w_v), fade_widen, anchor, sums,
        partial, reach, late_whole,
    )
    early_recept = recept_early(where, pieces, diffs, hidden, ratios, widen, w_r)
    middle, end = LAST // SUB, x.shape[0] // SUB
    jobs = (
        (early_recept, early, decay, tuple(range(middle)), 0),
        (late_recept, late, late_decay, tuple(range(middle, end)), LAST),
    )
    outputs = []
    for job in jobs:
        outputs.append(local_outputs(where, sums, reward, entering, offsets, *job))
    before = None
    for axis in reversed(SEQ):
        received = []
        for k in range(1, lax.axis_size(axis)):
            received.append(xor_permute(packed, axis, k))
        place = 2 + SEQ.index(axis)
        if axis != SEQ[0]:
            whole, packed, before = merge(where, place, whole, before, received)
    locals_, queries = zip(*outputs)
    return finish(where, place, locals_, queries, gain, shift, whole, before, received)


def solution(mesh):
    torus = Mesh(mesh.devices.reshape(4, 4, 2, 2, 2), ("z", "x", "y_hi", "y_lo", "core"))
    placed = (
        P(SEQ, MP),
        P(SEQ),
        P(),
        P(MP, None),
        P(),
        P(MP, None),
        P(None, MP),
        P(MP),
        P(MP),
        P(None, MP),
        P(None, MP),
        P(None, MP),
        P(MP),
        P(MP),
    )
    return jax.shard_map(inner, mesh=torus, in_specs=placed, out_specs=P(SEQ, MP), check_vma=False)
```

```python
import functools

import jax
import jax.numpy as jnp
import numpy as np
from jax import lax
from jax.experimental import pallas as pl
from jax.experimental.pallas import tpu as pltpu
from jax.sharding import Mesh
from jax.sharding import PartitionSpec as P


F32 = jnp.float32
BF16 = jnp.bfloat16
GROUP = 64
SUB = 64
LAST = 256
SPLIT = 128
CTX = 16
HALVES = (32, 16, 8, 4, 2, 1)
FLOOR = -100.0
SEQ = ("z", "x", "y_hi")
MP = ("y_lo", "core")


def xor_permute(array, axes, flip):
    length = lax.axis_size(axes)
    return lax.ppermute(array, axes, [(i, i ^ flip) for i in range(length)])


def dot(a, b):
    return jnp.dot(a, b, preferred_element_type=F32)


def dot_nt(a, b):
    return lax.dot_general(a, b, (((1,), (1,)), ((), ())), preferred_element_type=F32)


def dot_tn(a, b):
    return lax.dot_general(a, b, (((0,), (0,)), ((), ())), preferred_element_type=F32)


def sum_rows():
    t = np.arange(SUB)[:, None]
    j = np.arange(SUB)[None, :]
    blocks = []
    for half in HALVES:
        middle = (t // (2 * half)) * (2 * half) + half - 1
        right = t > middle
        blocks.append(np.where(right, (j > middle) & (j < t), (j > t) & (j <= middle)))
    blocks.append(j < t)
    blocks.append(j > t)
    one = np.concatenate(blocks, 0)
    return np.concatenate([one, one], 1).astype(np.float32)


SMEM = pl.BlockSpec(memory_space=pltpu.SMEM)
VMEM = pl.BlockSpec(memory_space=pltpu.VMEM)


def in_hbm(array):
    return pltpu.with_memory_space_constraint(array, pltpu.HBM)


def in_vmem(array):
    return pltpu.with_memory_space_constraint(array, pltpu.VMEM)


def cut_kernel(where_ref, x, late_a, late_b, early, last, ready):
    tokens = x.shape[0]
    moves = (
        (x.at[LAST - CTX : LAST + SPLIT, :], late_a),
        (x.at[tokens - CTX :, :], last),
        (x.at[LAST + SPLIT :, :], late_b),
        (x.at[0:LAST, :], early.at[CTX:, :]),
    )
    copies = [pltpu.make_async_copy(a, b, ready.at[i]) for i, (a, b) in enumerate(moves)]
    for copy in copies:
        copy.start()
    early[0:CTX, :] = jnp.zeros((CTX, early.shape[1]), BF16)
    for copy in copies:
        copy.wait()


def cut(where, x):
    tokens, width = x.shape
    return pl.pallas_call(
        cut_kernel,
        in_specs=[SMEM, pl.BlockSpec(memory_space=pltpu.HBM)],
        out_specs=[VMEM] * 4,
        scratch_shapes=[pltpu.SemaphoreType.DMA((4,))],
        out_shape=[
            pltpu.VMEM((CTX + SPLIT, width), BF16),
            pltpu.VMEM((tokens - LAST - SPLIT, width), BF16),
            pltpu.VMEM((CTX + LAST, width), BF16),
            pltpu.VMEM((CTX, width), BF16),
        ],
        compiler_params=pltpu.CompilerParams(vmem_limit_bytes=2**20),
        cost_estimate=pl.CostEstimate(flops=10**6, bytes_accessed=2 * 10**6, transcendentals=0),
    )(where, in_hbm(x))


def load_kernel(where_ref, *refs, kinds):
    count = len(kinds)
    ready = refs[2 * count]
    copies = []
    for i, kind in enumerate(kinds):
        source, target = refs[i], refs[count + i]
        if kind == "plain":
            copies.append(pltpu.make_async_copy(source, target, ready.at[i, 0]))
            continue
        width = target.shape[-1] if kind == "lanes" else target.shape[1]
        for j in range(4):
            there = pl.ds(pl.multiple_of((where_ref[0] ^ j) * width, width), width)
            block = source.at[:, :, there] if kind == "lanes" else source.at[there, :]
            copies.append(pltpu.make_async_copy(block, target.at[j], ready.at[i, j]))
    for copy in copies:
        copy.start()
    for copy in copies:
        copy.wait()


def load(where, *jobs):
    kinds, arrays = zip(*jobs)
    shapes = []
    for kind, a in jobs:
        if kind == "rows":
            shapes.append((4, a.shape[0] // 4, a.shape[1]))
        elif kind == "lanes":
            shapes.append((4, *a.shape[:2], a.shape[2] // 4))
        else:
            shapes.append(a.shape)
    return pl.pallas_call(
        functools.partial(load_kernel, kinds=kinds),
        in_specs=[SMEM] + [pl.BlockSpec(memory_space=pltpu.HBM)] * len(jobs),
        out_specs=[VMEM] * len(jobs),
        scratch_shapes=[pltpu.SemaphoreType.DMA((len(jobs), 4))],
        out_shape=[pltpu.VMEM(shape, a.dtype) for shape, a in zip(shapes, arrays)],
        compiler_params=pltpu.CompilerParams(vmem_limit_bytes=2**20),
        cost_estimate=pl.CostEstimate(flops=3 * 10**9, bytes_accessed=8 * 10**6, transcendentals=0),
    )(where, *map(in_hbm, arrays))


def read_rows(refs, cols):
    parts = [ref[:, cols] for ref in refs]
    return parts[0] if len(parts) == 1 else jnp.concatenate(parts, 0)


def mix_rows(me, start, first_token, pieces, narrows, weights, diffs, slots, consume, branches=(0, 1, 2, 3), ranked=None):
    ratios, widen = weights
    tokens, width = diffs.shape[1:]
    tile = 256
    line = lax.broadcasted_iota(jnp.int32, (tokens, tile), 0)
    first = lax.broadcasted_iota(jnp.int32, (8, tile), 0) == 0
    opens = line + first_token == start

    rank = jnp.zeros((tokens, 256), F32)
    for j in range(4):
        base = (me ^ j) * width
        parts = []
        for n in range(width // tile):
            cols = slice(tile * n, tile * n + tile)
            rows = read_rows(pieces[j], cols).astype(F32)
            x = rows[CTX:]
            before = pltpu.roll(x, 1, 0)
            before = jnp.concatenate([jnp.where(first, rows[CTX - 1 : CTX], before[0:8]), before[8:]], 0)
            d = jnp.where(opens, 0.0, before) - x
            diffs[j, :, cols] = d
            ratio = ratios[0:1, pl.ds(pl.multiple_of(base + tile * n, tile), tile)]
            parts.append((x + d * ratio).astype(BF16))
        rank = rank + dot(jnp.concatenate(parts, 1), narrows[j][...])
    if ranked:
        ranked()
    total = jnp.tanh(rank).astype(BF16)
    hidden = [total[:, 64 * b : 64 * b + 64] for b in range(4)]

    def mix(j):
        base = (me ^ j) * width
        for n in range(width // tile):
            cols = slice(tile * n, tile * n + tile)
            there = pl.ds(pl.multiple_of(base + tile * n, tile), tile)
            x = read_rows(pieces[j], cols)[CTX:].astype(F32)
            d = diffs[j, :, cols]
            for b in branches:
                delta = dot(hidden[b], widen[j, b, :, cols])
                slots(j, b)[:, cols] = (x + d * (ratios[b + 1 : b + 2, there] + delta)).astype(BF16)

    mix(0)
    for j in range(4):
        if j < 3:
            mix(j + 1)
        consume(j)
    return hidden


def add_product(out, cols, j, rows, weights):
    part = dot(rows[...], weights[j])
    if j == 0:
        out[:, cols] = part
    else:
        out[:, cols] += part


def decay_of(low, fade_widen, anchor):
    return -jnp.exp(anchor[...] + dot(jnp.tanh(low).astype(BF16), fade_widen[...]))


def take_pieces(refs, counts):
    pieces = []
    for count in counts:
        pieces.append(refs[:count])
        refs = refs[count:]
    return pieces, refs


def late_kernel(where_ref, *refs, counts):
    pieces, refs = take_pieces(refs, counts)
    narrows, refs = refs[0:4], refs[4:]
    ratios, widen, w_k_far, w_v_far, w_r_far, pair, recept, fading_rows, w_k, w_v, w_r, diffs, mixed, ready = refs
    channels, width = recept.shape[1], w_k.shape[1]

    def fetch(j, i):
        there = pl.ds(pl.multiple_of((where_ref[0] ^ j) * width, width), width)
        source, target = ((w_k_far, w_k), (w_v_far, w_v), (w_r_far, w_r))[i]
        return pltpu.make_async_copy(source.at[there, :], target.at[j], ready.at[j, i])

    def start_fetches(j):
        for i in range(3):
            fetch(j, i).start()

    start_fetches(0)
    start_fetches(1)

    def slots(j, b):
        return fading_rows.at[j] if b == 0 else mixed.at[j % 2, b - 1]

    def consume(j):
        fetch(j, 0).wait()
        add_product(pair, slice(0, channels), j, slots(j, 1), w_k)
        fetch(j, 1).wait()
        add_product(pair, slice(channels, 2 * channels), j, slots(j, 2), w_v)
        fetch(j, 2).wait()
        add_product(recept, slice(None), j, slots(j, 3), w_r)

    def ranked():
        start_fetches(2)
        start_fetches(3)

    mix_rows(where_ref[0], where_ref[1], LAST, pieces, narrows, (ratios, widen), diffs, slots, consume, ranked=ranked)


def decay_kernel(where_ref, rows, *refs):
    fadings, (fade_widen, anchor, sums, pair, out, partial, reach, whole) = refs[0:4], refs[4:]
    tokens, _ = out.shape
    low = dot(rows[0], fadings[0][...])
    for j in range(1, 4):
        low = low + dot(rows[j], fadings[j][...])
    out[...] = decay_of(low, fade_widen, anchor)
    count = tokens // SUB

    def note(n, state, decay, offset):
        partial[n] = state
        reach[n : n + 1, :] = decay
        reach[count + n : count + n + 1, :] = offset

    numbers = range(LAST // SUB, LAST // SUB + count)
    state, decay, _ = add_states(where_ref[1], sums, pair, out, numbers, LAST, note)
    store(whole, decay, state)


def early_kernel(where_ref, *refs, counts):
    pieces, refs = take_pieces(refs, counts)
    narrows, fadings, refs = refs[0:4], refs[4:8], refs[8:]
    ratios, widen, w_k, w_v, fade_widen, anchor, sums, partial, reach, late_whole = refs[:10]
    pair, decay, entering, offsets, whole, packed, diffs, hidden, mixed = refs[10:]
    channels = decay.shape[1]
    low = [None]

    def slots(j, b):
        return mixed.at[j % 2, b]

    def consume(j):
        part = dot(slots(j, 0)[...], fadings[j][...])
        low[0] = part if j == 0 else low[0] + part
        add_product(pair, slice(0, channels), j, slots(j, 1), w_k)
        add_product(pair, slice(channels, 2 * channels), j, slots(j, 2), w_v)

    ranks = mix_rows(
        where_ref[0], where_ref[1], 0, pieces, narrows, (ratios, widen), diffs, slots, consume, branches=(0, 1, 2)
    )
    hidden[...] = ranks[3]
    decay[...] = decay_of(low[0], fade_widen, anchor)

    def note(n, state, _, offset):
        entering[n] = state.astype(BF16)
        offsets[n : n + 1, :] = offset

    count, more = LAST // SUB, partial.shape[0]
    state, total, offset = add_states(where_ref[1], sums, pair, decay, range(count), 0, note)
    final = combine((total, state), (late_whole[SUB : SUB + 1], late_whole[0:SUB]))
    store(whole, *final)
    pack(packed, *final)
    for n in range(more):
        entering[count + n] = (partial[n] + reach[n : n + 1, :] * state).astype(BF16)
        offsets[count + n : count + n + 1, :] = offset + reach[more + n : more + n + 1, :]


def recept_kernel(where_ref, *refs, counts):
    pieces, refs = take_pieces(refs, counts)
    diffs, hidden, ratios, widen, w_r, out, mixed = refs
    width = diffs.shape[2]
    tile = 256
    for j in range(4):
        base = (where_ref[0] ^ j) * width
        for n in range(width // tile):
            cols = slice(tile * n, tile * n + tile)
            there = pl.ds(pl.multiple_of(base + tile * n, tile), tile)
            x = read_rows(pieces[j], cols)[CTX:].astype(F32)
            delta = dot(hidden[...], widen[j, 3, :, cols])
            mixed[j, :, cols] = (x + diffs[j, :, cols] * (ratios[4:5, there] + delta)).astype(BF16)
        add_product(out, slice(None), j, mixed.at[j], w_r)


def recept_early(where, pieces, diffs, hidden, ratios, widen, w_r):
    tokens, width = diffs.shape[1:]
    counts = tuple(len(p) for p in pieces)
    operands = [a for p in pieces for a in p]
    return pl.pallas_call(
        functools.partial(recept_kernel, counts=counts),
        in_specs=[SMEM] + [VMEM] * (len(operands) + 5),
        out_specs=VMEM,
        scratch_shapes=[pltpu.VMEM((4, tokens, width), BF16)],
        out_shape=pltpu.VMEM((tokens, w_r.shape[2]), F32),
        compiler_params=pltpu.CompilerParams(vmem_limit_bytes=7 * 2**20),
        cost_estimate=pl.CostEstimate(flops=2 * 10**9, bytes_accessed=5 * 10**6, transcendentals=0),
    )(where, *operands, *map(in_vmem, (diffs, hidden, ratios, widen, w_r)))


def project_late(where, pieces, narrows, ratios, widen, w_k, w_v, w_r):
    width, channels = w_k.shape[0] // 4, w_k.shape[1]
    counts = tuple(len(p) for p in pieces)
    tokens = sum(a.shape[0] for a in pieces[0]) - CTX
    operands = [a for p in pieces for a in p] + narrows
    return pl.pallas_call(
        functools.partial(late_kernel, counts=counts),
        in_specs=[SMEM] + [VMEM] * (len(operands) + 2) + [pl.BlockSpec(memory_space=pltpu.HBM)] * 3,
        out_specs=[VMEM] * 6,
        scratch_shapes=[
            pltpu.VMEM((4, tokens, width), F32),
            pltpu.VMEM((2, 3, tokens, width), BF16),
            pltpu.SemaphoreType.DMA((4, 3)),
        ],
        out_shape=[
            pltpu.VMEM((tokens, 2 * channels), F32),
            pltpu.VMEM((tokens, channels), F32),
            pltpu.VMEM((4, tokens, width), BF16),
            pltpu.VMEM((4, width, channels), BF16),
            pltpu.VMEM((4, width, channels), BF16),
            pltpu.VMEM((4, width, channels), BF16),
        ],
        compiler_params=pltpu.CompilerParams(vmem_limit_bytes=(4 * 1024 + 40 * tokens) * 1024),
        cost_estimate=pl.CostEstimate(flops=25 * 10**6 * tokens, bytes_accessed=17 * 10**6, transcendentals=0),
    )(where, *operands, *map(in_vmem, (ratios, widen)), *map(in_hbm, (w_k, w_v, w_r)))


def decay_late(where, rows, fadings, fade_widen, anchor, sums, pair):
    tokens, channels = rows.shape[1], anchor.shape[1]
    count = tokens // SUB
    return pl.pallas_call(
        decay_kernel,
        in_specs=[SMEM] + [VMEM] * 9,
        out_specs=[VMEM] * 4,
        out_shape=[
            pltpu.VMEM((tokens, channels), F32),
            pltpu.VMEM((count, SUB, channels), F32),
            pltpu.VMEM((2 * count, channels), F32),
            pltpu.VMEM((SUB + 8, channels), F32),
        ],
        compiler_params=pltpu.CompilerParams(vmem_limit_bytes=5 * 2**20),
        cost_estimate=pl.CostEstimate(flops=10**9, bytes_accessed=2 * 10**6, transcendentals=0),
    )(where, in_vmem(rows), *fadings, *map(in_vmem, (fade_widen, anchor, sums, pair)))


def project_early(where, pieces, narrows, fadings, weights, *rest):
    width, channels = weights[2].shape[1:]
    counts = tuple(len(p) for p in pieces)
    operands = [a for p in pieces for a in p] + narrows + fadings
    return pl.pallas_call(
        functools.partial(early_kernel, counts=counts),
        in_specs=[SMEM] + [VMEM] * (len(operands) + len(weights) + len(rest)),
        out_specs=[VMEM] * 8,
        scratch_shapes=[pltpu.VMEM((2, 3, LAST, width), BF16)],
        out_shape=[
            pltpu.VMEM((LAST, 2 * channels), F32),
            pltpu.VMEM((LAST, channels), F32),
            pltpu.VMEM((8, SUB, channels), BF16),
            pltpu.VMEM((8, channels), F32),
            jax.ShapeDtypeStruct((SUB + 8, channels), F32),
            jax.ShapeDtypeStruct((SUB + 8, channels), BF16),
            pltpu.VMEM((4, LAST, width), F32),
            pltpu.VMEM((LAST, 64), BF16),
        ],
        compiler_params=pltpu.CompilerParams(vmem_limit_bytes=(5 * 1024 + 16 * LAST) * 1024),
        cost_estimate=pl.CostEstimate(flops=25 * 10**6 * LAST, bytes_accessed=17 * 10**6, transcendentals=0),
    )(where, *operands, *map(in_vmem, (*weights, *rest)))


def split_two(w):
    high = w.astype(BF16)
    low = (w - high.astype(F32)).astype(BF16)
    return jnp.concatenate([high, low], 0)


def add_states(start, sums, pair, decays, numbers, first_token, note):
    channels = decays.shape[1]
    line = lax.broadcasted_iota(jnp.int32, (SUB, 1), 0)
    lane = lax.broadcasted_iota(jnp.int32, (SUB, 128), 1)
    state = jnp.zeros((SUB, channels), F32)
    decay = jnp.ones((1, channels), F32)
    offset = jnp.zeros((1, channels), F32)
    for n, c in enumerate(numbers):
        note(n, state, decay, offset)
        at = SUB * c - first_token
        w = jnp.maximum(decays[at : at + SUB, :], FLOOR)
        k = pair[at : at + SUB, 0:channels]
        v = pair[at : at + SUB, channels : 2 * channels].astype(BF16)
        tail = dot(sums[7 * SUB : 8 * SUB, :], split_two(w))
        ends_late = (c * SUB + SUB - 1) >= start
        begins_late = (c * SUB - 1) >= start if c else jnp.bool_(False)
        late = (line + c * SUB) >= start
        log_total = tail[0:1, :] + w[0:1, :]
        total = jnp.where(begins_late == ends_late, jnp.exp(log_total), 0.0)
        kk = jnp.where(late == ends_late, k * jnp.exp(tail), 0.0).astype(BF16)
        pieces = []
        for p in range(channels // 128):
            cols = slice(128 * p, 128 * p + 128)
            both = dot_tn(v[:, cols], kk[:, cols])
            pieces.append(jnp.where(lane < GROUP, both[0:GROUP], both[GROUP:128]))
        state = state * total + jnp.concatenate(pieces, 1)
        decay = decay * total
        offset = offset + log_total
    return state, decay, offset


def local_kernel(where_ref, sums, reward, entering, offsets, recept, pair, decay, local, queries, *, first, count, first_token):
    start = where_ref[1]
    channels = local.shape[1]
    line = lax.broadcasted_iota(jnp.int32, (SUB, 1), 0)
    lane = lax.broadcasted_iota(jnp.int32, (SUB, 128), 1)
    two_t = lax.broadcasted_iota(jnp.int32, (2 * SUB, SUB), 0) % SUB
    two_s = lax.broadcasted_iota(jnp.int32, (2 * SUB, SUB), 1)

    def apart(a):
        zero = jnp.zeros_like(a)
        return jnp.concatenate([jnp.where(lane < GROUP, a, zero), jnp.where(lane < GROUP, zero, a)], 0)

    for n in range(count):
        c = first + n
        at = SUB * c - first_token
        there = slice(at, at + SUB)
        r = recept[there, :]
        k, v = [pair[there, channels * i : channels * i + channels] for i in range(2)]
        w = decay[there, :]
        v = v.astype(BF16)
        w = jnp.maximum(w, FLOOR)
        sides = []
        exponents = dot(sums[0 : 7 * SUB, :], split_two(w))
        for level, half in enumerate(HALVES):
            right = (line // half) % 2 == 1
            e = jnp.exp(exponents[SUB * level : SUB * level + SUB, :])
            sides.append((jnp.where(right, r, k) * e).astype(BF16))
        before_here = exponents[6 * SUB : 7 * SUB, :]
        late = (line + c * SUB) >= start
        begins_late = (c * SUB - 1) >= start if c else jnp.bool_(False)
        reach = jnp.where(late == begins_late, r * jnp.exp(before_here), 0.0).astype(BF16)
        offset = offsets[c : c + 1, :]
        rows = slice(SUB * n, SUB * n + SUB)
        queries[rows, :] = jnp.where(late, 0.0, r * jnp.exp(offset + before_here)).astype(BF16)
        own = (r * reward[...]).astype(BF16)
        k_own = k.astype(BF16)
        same = ((two_t + c * SUB) >= start) == ((two_s + c * SUB) >= start)
        for p in range(channels // 128):
            cols = slice(128 * p, 128 * p + 128)
            scores = jnp.where(two_t == two_s, dot_nt(apart(own[:, cols]), k_own[:, cols]), 0.0)
            for level, half in enumerate(HALVES):
                side = sides[level][:, cols]
                part = dot_nt(apart(side), side)
                here = (two_t // (2 * half) == two_s // (2 * half)) & ((two_t // half) % 2 == 1) & ((two_s // half) % 2 == 0)
                scores = jnp.where(here & same, part, scores)
            both = dot(scores.astype(BF16), v[:, cols])
            out = jnp.where(lane < GROUP, both[0:SUB], both[SUB : 2 * SUB])
            local[rows, cols] = out + dot_nt(reach[:, cols], apart(entering[c, :, cols]))


def local_outputs(where, sums, reward, entering, offsets, recept, pair, decay, numbers, first_token):
    channels = entering.shape[2]
    tokens = len(numbers) * SUB
    return pl.pallas_call(
        functools.partial(local_kernel, first=numbers[0], count=len(numbers), first_token=first_token),
        in_specs=[SMEM] + [VMEM] * 7,
        out_specs=[VMEM] * 2,
        out_shape=[pltpu.VMEM((tokens, channels), F32), pltpu.VMEM((tokens, channels), BF16)],
        compiler_params=pltpu.CompilerParams(vmem_limit_bytes=8 * 1024 * 1024),
        cost_estimate=pl.CostEstimate(flops=2 * 10**9, bytes_accessed=3 * 10**6, transcendentals=0),
    )(where, *map(in_vmem, (sums, reward, entering, offsets, recept, pair, decay)))


def unpack(ref):
    return ref[SUB : SUB + 1].astype(F32) + ref[SUB + 1 : SUB + 2].astype(F32), ref[0:SUB].astype(F32)


def pack(ref, decay, state):
    high = decay.astype(BF16)
    low = (decay - high.astype(F32)).astype(BF16)
    wide = (8, decay.shape[1])
    line = lax.broadcasted_iota(jnp.int32, wide, 0)
    high, low = high.astype(F32), low.astype(F32)
    ref[0:SUB, :] = state.astype(BF16)
    ref[SUB : SUB + 8, :] = jnp.where(line == 0, high, jnp.where(line == 1, low, 0.0)).astype(BF16)


def store(ref, decay, state):
    ref[0:SUB, :] = state
    ref[SUB : SUB + 8, :] = jnp.broadcast_to(decay, (8, decay.shape[1]))


def combine(earlier, later):
    return earlier[0] * later[0], later[0] * earlier[1] + later[1]


def choose(flag, a, b):
    return tuple(jnp.where(flag, u, v) for u, v in zip(a, b))


def along_axis(here, own, received, before):
    pieces = [own] + [unpack(ref) for ref in received]
    length = len(pieces)
    start = (jnp.ones_like(own[0]), jnp.zeros_like(own[1]))
    inside, so_far = start, None
    for m in range(length):
        from_m = pieces[m]
        for other in range(1, length):
            from_m = choose(here == other, pieces[m ^ other], from_m)
        if m:
            inside = choose(here == m, so_far, inside)
        so_far = from_m if so_far is None else combine(so_far, from_m)
    return inside if before is None else combine(inside, before), so_far


def merge_kernel(where_ref, *refs, place, count, opening):
    whole, refs = refs[0], refs[1:]
    before = None
    if not opening:
        before, refs = (refs[0][SUB : SUB + 1], refs[0][0:SUB]), refs[1:]
    received, (whole_out, packed_out, before_out) = refs[:count], refs[count:]
    own = (whole[SUB : SUB + 1], whole[0:SUB])
    before, total = along_axis(where_ref[place], own, received, before)
    store(whole_out, *total)
    pack(packed_out, *total)
    store(before_out, *before)


def merge(where, place, whole, before, received):
    channels = whole.shape[1]
    operands = [whole] + ([] if before is None else [before]) + received
    return pl.pallas_call(
        functools.partial(merge_kernel, place=place, count=len(received), opening=before is None),
        in_specs=[SMEM] + [VMEM] * len(operands),
        out_specs=[VMEM] * 3,
        out_shape=[
            jax.ShapeDtypeStruct((SUB + 8, channels), F32),
            jax.ShapeDtypeStruct((SUB + 8, channels), BF16),
            jax.ShapeDtypeStruct((SUB + 8, channels), F32),
        ],
        compiler_params=pltpu.CompilerParams(vmem_limit_bytes=4 * 1024 * 1024),
        cost_estimate=pl.CostEstimate(flops=10**8, bytes_accessed=10**6, transcendentals=0),
    )(where, *operands)


def finish_kernel(where_ref, *refs, parts, place):
    locals_, queries, refs = refs[:parts], refs[parts : 2 * parts], refs[2 * parts :]
    gain, shift, whole, before, *received, out, held, ready = refs
    own = (whole[SUB : SUB + 1], whole[0:SUB])
    (_, incoming), _ = along_axis(where_ref[place], own, received, (before[SUB : SUB + 1], before[0:SUB]))
    incoming = incoming.astype(BF16)
    channels = gain.shape[1]
    wide = 256
    lane = lax.broadcasted_iota(jnp.int32, (SUB, wide), 1) // GROUP
    row = lax.broadcasted_iota(jnp.int32, (wide, wide), 0)
    col = lax.broadcasted_iota(jnp.int32, (wide, wide), 1)
    average = jnp.where((row // GROUP) == (col // GROUP), 1.0 / GROUP, 0.0).astype(BF16)
    blocks = []
    for p in range(channels // wide):
        st = incoming[:, wide * p : wide * p + wide]
        blocks.append(jnp.concatenate([jnp.where(lane == h, st, jnp.zeros_like(st)) for h in range(wide // GROUP)], 0))
    copies = []
    at = 0
    for i in range(parts):
        rows = slice(at, at + locals_[i].shape[0])
        at = rows.stop
        for p in range(channels // wide):
            cols = slice(wide * p, wide * p + wide)
            o = locals_[i][:, cols] + dot_nt(queries[i][:, cols], blocks[p])
            centred = o - dot(o.astype(BF16), average)
            variance = dot((centred * centred).astype(BF16), average)
            normed = centred * lax.rsqrt(variance + 0.00064)
            held[rows, cols] = (normed * gain[:, cols] + shift[:, cols]).astype(BF16)
        copies.append(pltpu.make_async_copy(held.at[rows, :], out.at[rows, :], ready.at[i]))
        copies[-1].start()
    for copy in copies:
        copy.wait()


def finish(where, place, locals_, queries, gain, shift, whole, before, received):
    parts = len(locals_)
    tokens, channels = sum(a.shape[0] for a in locals_), gain.shape[1]
    return pl.pallas_call(
        functools.partial(finish_kernel, parts=parts, place=place),
        in_specs=[SMEM] + [VMEM] * (2 * parts + 4 + len(received)),
        out_specs=pl.BlockSpec(memory_space=pltpu.HBM),
        scratch_shapes=[pltpu.VMEM((tokens, channels), BF16), pltpu.SemaphoreType.DMA((parts,))],
        out_shape=jax.ShapeDtypeStruct((tokens, channels), BF16),
        compiler_params=pltpu.CompilerParams(vmem_limit_bytes=8 * 1024 * 1024),
        cost_estimate=pl.CostEstimate(flops=10**9, bytes_accessed=2 * 10**6, transcendentals=0),
    )(where, *map(in_vmem, (*locals_, *queries, gain, shift)), whole, before, *received)


def inner(
    layer_inputs,
    article_opening,
    blending_ratios,
    blending_narrow_operand,
    blending_widen_operand,
    fading_narrow_operand,
    fading_widen_operand,
    fading_anchor,
    immediate_reward,
    acceptance_weights,
    lookup_weights,
    payload_weights,
    group_scaling_weight,
    group_scaling_shift,
):
    x = layer_inputs
    places = [lax.axis_index(axis).astype(jnp.int32) for axis in (MP, *SEQ)]
    where = jnp.stack([places[0], article_opening[0], *places[1:]])
    shards = lax.axis_size(SEQ)

    def across_far(a):
        return lax.ppermute(a, ("y_hi", "y_lo"), [(i, i ^ 3) for i in range(4)])

    def partner(a):
        return xor_permute(a, MP, 1)

    def across(a):
        return xor_permute(a, MP, 2)

    late_a, late_b, own_early, last = cut(where, x)
    own_late = [late_a, late_b]
    far_late_a = across(late_a)
    far_narrow = across_far(blending_narrow_operand)
    near_narrow = partner(blending_narrow_operand)
    far_fading = across_far(fading_narrow_operand)
    near_fading = partner(fading_narrow_operand)
    near_late_a = partner(late_a)
    before = lax.ppermute(last, SEQ, [(i, i + 1) for i in range(shards - 1)])
    far_late_b = across(late_b)
    near_late_b = partner(late_b)
    own_early = lax.dynamic_update_slice(own_early, before, (0, 0))
    far_early = across(own_early)
    near_early = partner(own_early)
    sums = jnp.asarray(sum_rows(), BF16)
    widen, ratios, narrow, fade_widen, anchor, sums, reward, gain, shift, fading = load(
        where, ("lanes", blending_widen_operand), ("plain", blending_ratios),
        ("plain", blending_narrow_operand), ("plain", fading_widen_operand), ("plain", fading_anchor[None]),
        ("plain", sums), ("plain", immediate_reward[None]), ("plain", group_scaling_weight[None]),
        ("plain", group_scaling_shift[None]), ("plain", fading_narrow_operand),
    )
    next_late_a = partner(far_late_a)
    next_narrow = partner(far_narrow)
    next_fading = partner(far_fading)
    next_late_b = partner(far_late_b)
    narrows = [narrow, near_narrow, far_narrow, next_narrow]
    fadings = [fading, near_fading, far_fading, next_fading]
    pieces = [own_late, [near_late_a, near_late_b], [far_late_a, far_late_b], [next_late_a, next_late_b]]
    late, late_recept, fading_rows, w_k, w_v, w_r = project_late(
        where, pieces, narrows, ratios, widen, lookup_weights, payload_weights, acceptance_weights
    )
    far_early, late = lax.optimization_barrier((far_early, late))
    late_decay, partial, reach, late_whole = decay_late(where, fading_rows, fadings, fade_widen, anchor, sums, late)
    next_early = partner(far_early)
    pieces = [[own_early], [near_early], [far_early], [next_early]]
    early, decay, entering, offsets, whole, packed, diffs, hidden = project_early(
        where, pieces, narrows, fadings, (ratios, widen, w_k, w_v), fade_widen, anchor, sums,
        partial, reach, late_whole,
    )
    early_recept = recept_early(where, pieces, diffs, hidden, ratios, widen, w_r)
    middle, end = LAST // SUB, x.shape[0] // SUB
    jobs = (
        (early_recept, early, decay, tuple(range(middle)), 0),
        (late_recept, late, late_decay, tuple(range(middle, end)), LAST),
    )
    outputs = []
    for job in jobs:
        outputs.append(local_outputs(where, sums, reward, entering, offsets, *job))
    before = None
    for axis in reversed(SEQ):
        received = []
        for k in range(1, lax.axis_size(axis)):
            received.append(xor_permute(packed, axis, k))
        place = 2 + SEQ.index(axis)
        if axis != SEQ[0]:
            whole, packed, before = merge(where, place, whole, before, received)
    locals_, queries = zip(*outputs)
    return finish(where, place, locals_, queries, gain, shift, whole, before, received)


def solution(mesh):
    torus = Mesh(mesh.devices.reshape(4, 4, 2, 2, 2), ("z", "x", "y_hi", "y_lo", "core"))
    placed = (
        P(SEQ, MP),
        P(SEQ),
        P(),
        P(MP, None),
        P(),
        P(MP, None),
        P(None, MP),
        P(MP),
        P(MP),
        P(None, MP),
        P(None, MP),
        P(None, MP),
        P(MP),
        P(MP),
    )
    return jax.shard_map(inner, mesh=torus, in_specs=placed, out_specs=P(SEQ, MP), check_vma=False)
```

```python
import functools

import jax
import jax.numpy as jnp
import numpy as np
from jax import lax
from jax.experimental import pallas as pl
from jax.experimental.pallas import tpu as pltpu
from jax.sharding import Mesh
from jax.sharding import PartitionSpec as P


F32 = jnp.float32
BF16 = jnp.bfloat16
GROUP = 64
SUB = 64
LAST = 256
SPLIT = 128
CTX = 16
HALVES = (32, 16, 8, 4, 2, 1)
FLOOR = -100.0
SEQ = ("z", "x", "y_hi")
MP = ("y_lo", "core")


def xor_permute(array, axes, flip):
    length = lax.axis_size(axes)
    return lax.ppermute(array, axes, [(i, i ^ flip) for i in range(length)])


def dot(a, b):
    return jnp.dot(a, b, preferred_element_type=F32)


def dot_nt(a, b):
    return lax.dot_general(a, b, (((1,), (1,)), ((), ())), preferred_element_type=F32)


def dot_tn(a, b):
    return lax.dot_general(a, b, (((0,), (0,)), ((), ())), preferred_element_type=F32)


def sum_rows():
    t = np.arange(SUB)[:, None]
    j = np.arange(SUB)[None, :]
    blocks = []
    for half in HALVES:
        middle = (t // (2 * half)) * (2 * half) + half - 1
        right = t > middle
        blocks.append(np.where(right, (j > middle) & (j < t), (j > t) & (j <= middle)))
    blocks.append(j < t)
    blocks.append(j > t)
    one = np.concatenate(blocks, 0)
    return np.concatenate([one, one], 1).astype(np.float32)


SMEM = pl.BlockSpec(memory_space=pltpu.SMEM)
VMEM = pl.BlockSpec(memory_space=pltpu.VMEM)


def in_hbm(array):
    return pltpu.with_memory_space_constraint(array, pltpu.HBM)


def in_vmem(array):
    return pltpu.with_memory_space_constraint(array, pltpu.VMEM)


def cut_kernel(where_ref, x, late_a, late_b, early, last, ready):
    tokens = x.shape[0]
    moves = (
        (x.at[LAST - CTX : LAST + SPLIT, :], late_a),
        (x.at[tokens - CTX :, :], last),
        (x.at[LAST + SPLIT :, :], late_b),
        (x.at[0:LAST, :], early.at[CTX:, :]),
    )
    copies = [pltpu.make_async_copy(a, b, ready.at[i]) for i, (a, b) in enumerate(moves)]
    for copy in copies:
        copy.start()
    early[0:CTX, :] = jnp.zeros((CTX, early.shape[1]), BF16)
    for copy in copies:
        copy.wait()


def cut(where, x):
    tokens, width = x.shape
    return pl.pallas_call(
        cut_kernel,
        in_specs=[SMEM, pl.BlockSpec(memory_space=pltpu.HBM)],
        out_specs=[VMEM] * 4,
        scratch_shapes=[pltpu.SemaphoreType.DMA((4,))],
        out_shape=[
            pltpu.VMEM((CTX + SPLIT, width), BF16),
            pltpu.VMEM((tokens - LAST - SPLIT, width), BF16),
            pltpu.VMEM((CTX + LAST, width), BF16),
            pltpu.VMEM((CTX, width), BF16),
        ],
        compiler_params=pltpu.CompilerParams(vmem_limit_bytes=2**20),
        cost_estimate=pl.CostEstimate(flops=10**6, bytes_accessed=2 * 10**6, transcendentals=0),
    )(where, in_hbm(x))


def load_kernel(where_ref, *refs, kinds):
    count = len(kinds)
    ready = refs[2 * count]
    copies = []
    for i, kind in enumerate(kinds):
        source, target = refs[i], refs[count + i]
        if kind == "plain":
            copies.append(pltpu.make_async_copy(source, target, ready.at[i, 0]))
            continue
        width = target.shape[-1] if kind == "lanes" else target.shape[1]
        for j in range(4):
            there = pl.ds(pl.multiple_of((where_ref[0] ^ j) * width, width), width)
            block = source.at[:, :, there] if kind == "lanes" else source.at[there, :]
            copies.append(pltpu.make_async_copy(block, target.at[j], ready.at[i, j]))
    for copy in copies:
        copy.start()
    for copy in copies:
        copy.wait()


def load(where, *jobs):
    kinds, arrays = zip(*jobs)
    shapes = []
    for kind, a in jobs:
        if kind == "rows":
            shapes.append((4, a.shape[0] // 4, a.shape[1]))
        elif kind == "lanes":
            shapes.append((4, *a.shape[:2], a.shape[2] // 4))
        else:
            shapes.append(a.shape)
    return pl.pallas_call(
        functools.partial(load_kernel, kinds=kinds),
        in_specs=[SMEM] + [pl.BlockSpec(memory_space=pltpu.HBM)] * len(jobs),
        out_specs=[VMEM] * len(jobs),
        scratch_shapes=[pltpu.SemaphoreType.DMA((len(jobs), 4))],
        out_shape=[pltpu.VMEM(shape, a.dtype) for shape, a in zip(shapes, arrays)],
        compiler_params=pltpu.CompilerParams(vmem_limit_bytes=2**20),
        cost_estimate=pl.CostEstimate(flops=3 * 10**9, bytes_accessed=8 * 10**6, transcendentals=0),
    )(where, *map(in_hbm, arrays))


def read_rows(refs, cols):
    parts = [ref[:, cols] for ref in refs]
    return parts[0] if len(parts) == 1 else jnp.concatenate(parts, 0)


def mix_rows(me, start, first_token, pieces, narrows, weights, diffs, slots, consume, branches=(0, 1, 2, 3), ranked=None):
    ratios, widen = weights
    tokens, width = diffs.shape[1:]
    tile = 256
    line = lax.broadcasted_iota(jnp.int32, (tokens, tile), 0)
    first = lax.broadcasted_iota(jnp.int32, (8, tile), 0) == 0
    opens = line + first_token == start

    rank = jnp.zeros((tokens, 256), F32)
    for j in range(4):
        base = (me ^ j) * width
        parts = []
        for n in range(width // tile):
            cols = slice(tile * n, tile * n + tile)
            rows = read_rows(pieces[j], cols).astype(F32)
            x = rows[CTX:]
            before = pltpu.roll(x, 1, 0)
            before = jnp.concatenate([jnp.where(first, rows[CTX - 1 : CTX], before[0:8]), before[8:]], 0)
            d = jnp.where(opens, 0.0, before) - x
            diffs[j, :, cols] = d
            ratio = ratios[0:1, pl.ds(pl.multiple_of(base + tile * n, tile), tile)]
            parts.append((x + d * ratio).astype(BF16))
        rank = rank + dot(jnp.concatenate(parts, 1), narrows[j][...])
    if ranked:
        ranked()
    total = jnp.tanh(rank).astype(BF16)
    hidden = [total[:, 64 * b : 64 * b + 64] for b in range(4)]

    def mix(j):
        base = (me ^ j) * width
        for n in range(width // tile):
            cols = slice(tile * n, tile * n + tile)
            there = pl.ds(pl.multiple_of(base + tile * n, tile), tile)
            x = read_rows(pieces[j], cols)[CTX:].astype(F32)
            d = diffs[j, :, cols]
            for b in branches:
                delta = dot(hidden[b], widen[j, b, :, cols])
                slots(j, b)[:, cols] = (x + d * (ratios[b + 1 : b + 2, there] + delta)).astype(BF16)

    mix(0)
    for j in range(4):
        if j < 3:
            mix(j + 1)
        consume(j)
    return hidden


def add_product(out, cols, j, rows, weights):
    part = dot(rows[...], weights[j])
    if j == 0:
        out[:, cols] = part
    else:
        out[:, cols] += part


def decay_of(low, fade_widen, anchor):
    return -jnp.exp(anchor[...] + dot(jnp.tanh(low).astype(BF16), fade_widen[...]))


def take_pieces(refs, counts):
    pieces = []
    for count in counts:
        pieces.append(refs[:count])
        refs = refs[count:]
    return pieces, refs


def late_kernel(where_ref, *refs, counts):
    pieces, refs = take_pieces(refs, counts)
    narrows, refs = refs[0:4], refs[4:]
    ratios, widen, w_k_far, w_v_far, w_r_far, pair, recept, fading_rows, w_k, w_v, w_r, diffs, mixed, ready = refs
    channels, width = recept.shape[1], w_k.shape[1]

    def fetch(j, i):
        there = pl.ds(pl.multiple_of((where_ref[0] ^ j) * width, width), width)
        source, target = ((w_k_far, w_k), (w_v_far, w_v), (w_r_far, w_r))[i]
        return pltpu.make_async_copy(source.at[there, :], target.at[j], ready.at[j, i])

    def start_fetches(j):
        for i in range(3):
            fetch(j, i).start()

    start_fetches(0)
    start_fetches(1)

    def slots(j, b):
        return fading_rows.at[j] if b == 0 else mixed.at[j % 2, b - 1]

    def consume(j):
        fetch(j, 0).wait()
        add_product(pair, slice(0, channels), j, slots(j, 1), w_k)
        fetch(j, 1).wait()
        add_product(pair, slice(channels, 2 * channels), j, slots(j, 2), w_v)
        fetch(j, 2).wait()
        add_product(recept, slice(None), j, slots(j, 3), w_r)

    def ranked():
        start_fetches(2)
        start_fetches(3)

    mix_rows(where_ref[0], where_ref[1], LAST, pieces, narrows, (ratios, widen), diffs, slots, consume, ranked=ranked)


def decay_kernel(where_ref, rows, *refs):
    fadings, (fade_widen, anchor, sums, pair, out, partial, reach, whole) = refs[0:4], refs[4:]
    tokens, _ = out.shape
    low = dot(rows[0], fadings[0][...])
    for j in range(1, 4):
        low = low + dot(rows[j], fadings[j][...])
    out[...] = decay_of(low, fade_widen, anchor)
    count = tokens // SUB

    def note(n, state, decay, offset):
        partial[n] = state
        reach[n : n + 1, :] = decay
        reach[count + n : count + n + 1, :] = offset

    numbers = range(LAST // SUB, LAST // SUB + count)
    state, decay, _ = add_states(where_ref[1], sums, pair, out, numbers, LAST, note)
    store(whole, decay, state)


def early_kernel(where_ref, *refs, counts):
    pieces, refs = take_pieces(refs, counts)
    narrows, fadings, refs = refs[0:4], refs[4:8], refs[8:]
    ratios, widen, w_k, w_v, fade_widen, anchor, sums, partial, reach, late_whole = refs[:10]
    pair, decay, entering, offsets, whole, packed, diffs, hidden, mixed = refs[10:]
    channels = decay.shape[1]
    low = [None]

    def slots(j, b):
        return mixed.at[j % 2, b]

    def consume(j):
        part = dot(slots(j, 0)[...], fadings[j][...])
        low[0] = part if j == 0 else low[0] + part
        add_product(pair, slice(0, channels), j, slots(j, 1), w_k)
        add_product(pair, slice(channels, 2 * channels), j, slots(j, 2), w_v)

    ranks = mix_rows(
        where_ref[0], where_ref[1], 0, pieces, narrows, (ratios, widen), diffs, slots, consume, branches=(0, 1, 2)
    )
    hidden[...] = ranks[3]
    decay[...] = decay_of(low[0], fade_widen, anchor)

    def note(n, state, _, offset):
        entering[n] = state.astype(BF16)
        offsets[n : n + 1, :] = offset

    count, more = LAST // SUB, partial.shape[0]
    state, total, offset = add_states(where_ref[1], sums, pair, decay, range(count), 0, note)
    final = combine((total, state), (late_whole[SUB : SUB + 1], late_whole[0:SUB]))
    store(whole, *final)
    pack(packed, *final)
    for n in range(more):
        entering[count + n] = (partial[n] + reach[n : n + 1, :] * state).astype(BF16)
        offsets[count + n : count + n + 1, :] = offset + reach[more + n : more + n + 1, :]


def recept_kernel(where_ref, *refs, counts):
    pieces, refs = take_pieces(refs, counts)
    diffs, hidden, ratios, widen, w_r, out, mixed = refs
    width = diffs.shape[2]
    tile = 256
    for j in range(4):
        base = (where_ref[0] ^ j) * width
        for n in range(width // tile):
            cols = slice(tile * n, tile * n + tile)
            there = pl.ds(pl.multiple_of(base + tile * n, tile), tile)
            x = read_rows(pieces[j], cols)[CTX:].astype(F32)
            delta = dot(hidden[...], widen[j, 3, :, cols])
            mixed[j, :, cols] = (x + diffs[j, :, cols] * (ratios[4:5, there] + delta)).astype(BF16)
        add_product(out, slice(None), j, mixed.at[j], w_r)


def recept_early(where, pieces, diffs, hidden, ratios, widen, w_r):
    tokens, width = diffs.shape[1:]
    counts = tuple(len(p) for p in pieces)
    operands = [a for p in pieces for a in p]
    return pl.pallas_call(
        functools.partial(recept_kernel, counts=counts),
        in_specs=[SMEM] + [VMEM] * (len(operands) + 5),
        out_specs=VMEM,
        scratch_shapes=[pltpu.VMEM((4, tokens, width), BF16)],
        out_shape=pltpu.VMEM((tokens, w_r.shape[2]), F32),
        compiler_params=pltpu.CompilerParams(vmem_limit_bytes=7 * 2**20),
        cost_estimate=pl.CostEstimate(flops=2 * 10**9, bytes_accessed=5 * 10**6, transcendentals=0),
    )(where, *operands, *map(in_vmem, (diffs, hidden, ratios, widen, w_r)))


def project_late(where, pieces, narrows, ratios, widen, w_k, w_v, w_r):
    width, channels = w_k.shape[0] // 4, w_k.shape[1]
    counts = tuple(len(p) for p in pieces)
    tokens = sum(a.shape[0] for a in pieces[0]) - CTX
    operands = [a for p in pieces for a in p] + narrows
    return pl.pallas_call(
        functools.partial(late_kernel, counts=counts),
        in_specs=[SMEM] + [VMEM] * (len(operands) + 2) + [pl.BlockSpec(memory_space=pltpu.HBM)] * 3,
        out_specs=[VMEM] * 6,
        scratch_shapes=[
            pltpu.VMEM((4, tokens, width), F32),
            pltpu.VMEM((2, 3, tokens, width), BF16),
            pltpu.SemaphoreType.DMA((4, 3)),
        ],
        out_shape=[
            pltpu.VMEM((tokens, 2 * channels), F32),
            pltpu.VMEM((tokens, channels), F32),
            pltpu.VMEM((4, tokens, width), BF16),
            pltpu.VMEM((4, width, channels), BF16),
            pltpu.VMEM((4, width, channels), BF16),
            pltpu.VMEM((4, width, channels), BF16),
        ],
        compiler_params=pltpu.CompilerParams(vmem_limit_bytes=(4 * 1024 + 40 * tokens) * 1024),
        cost_estimate=pl.CostEstimate(flops=25 * 10**6 * tokens, bytes_accessed=17 * 10**6, transcendentals=0),
    )(where, *operands, *map(in_vmem, (ratios, widen)), *map(in_hbm, (w_k, w_v, w_r)))


def decay_late(where, rows, fadings, fade_widen, anchor, sums, pair):
    tokens, channels = rows.shape[1], anchor.shape[1]
    count = tokens // SUB
    return pl.pallas_call(
        decay_kernel,
        in_specs=[SMEM] + [VMEM] * 9,
        out_specs=[VMEM] * 4,
        out_shape=[
            pltpu.VMEM((tokens, channels), F32),
            pltpu.VMEM((count, SUB, channels), F32),
            pltpu.VMEM((2 * count, channels), F32),
            pltpu.VMEM((SUB + 8, channels), F32),
        ],
        compiler_params=pltpu.CompilerParams(vmem_limit_bytes=5 * 2**20),
        cost_estimate=pl.CostEstimate(flops=10**9, bytes_accessed=2 * 10**6, transcendentals=0),
    )(where, in_vmem(rows), *fadings, *map(in_vmem, (fade_widen, anchor, sums, pair)))


def project_early(where, pieces, narrows, fadings, weights, *rest):
    width, channels = weights[2].shape[1:]
    counts = tuple(len(p) for p in pieces)
    operands = [a for p in pieces for a in p] + narrows + fadings
    return pl.pallas_call(
        functools.partial(early_kernel, counts=counts),
        in_specs=[SMEM] + [VMEM] * (len(operands) + len(weights) + len(rest)),
        out_specs=[VMEM] * 8,
        scratch_shapes=[pltpu.VMEM((2, 3, LAST, width), BF16)],
        out_shape=[
            pltpu.VMEM((LAST, 2 * channels), F32),
            pltpu.VMEM((LAST, channels), F32),
            pltpu.VMEM((8, SUB, channels), BF16),
            pltpu.VMEM((8, channels), F32),
            jax.ShapeDtypeStruct((SUB + 8, channels), F32),
            jax.ShapeDtypeStruct((SUB + 8, channels), BF16),
            pltpu.VMEM((4, LAST, width), F32),
            pltpu.VMEM((LAST, 64), BF16),
        ],
        compiler_params=pltpu.CompilerParams(vmem_limit_bytes=(5 * 1024 + 16 * LAST) * 1024),
        cost_estimate=pl.CostEstimate(flops=25 * 10**6 * LAST, bytes_accessed=17 * 10**6, transcendentals=0),
    )(where, *operands, *map(in_vmem, (*weights, *rest)))


def split_two(w):
    high = w.astype(BF16)
    low = (w - high.astype(F32)).astype(BF16)
    return jnp.concatenate([high, low], 0)


def add_states(start, sums, pair, decays, numbers, first_token, note):
    channels = decays.shape[1]
    line = lax.broadcasted_iota(jnp.int32, (SUB, 1), 0)
    lane = lax.broadcasted_iota(jnp.int32, (SUB, 128), 1)
    state = jnp.zeros((SUB, channels), F32)
    decay = jnp.ones((1, channels), F32)
    offset = jnp.zeros((1, channels), F32)
    for n, c in enumerate(numbers):
        note(n, state, decay, offset)
        at = SUB * c - first_token
        w = jnp.maximum(decays[at : at + SUB, :], FLOOR)
        k = pair[at : at + SUB, 0:channels]
        v = pair[at : at + SUB, channels : 2 * channels].astype(BF16)
        tail = dot(sums[7 * SUB : 8 * SUB, :], split_two(w))
        ends_late = (c * SUB + SUB - 1) >= start
        begins_late = (c * SUB - 1) >= start if c else jnp.bool_(False)
        late = (line + c * SUB) >= start
        log_total = tail[0:1, :] + w[0:1, :]
        total = jnp.where(begins_late == ends_late, jnp.exp(log_total), 0.0)
        kk = jnp.where(late == ends_late, k * jnp.exp(tail), 0.0).astype(BF16)
        pieces = []
        for p in range(channels // 128):
            cols = slice(128 * p, 128 * p + 128)
            both = dot_tn(v[:, cols], kk[:, cols])
            pieces.append(jnp.where(lane < GROUP, both[0:GROUP], both[GROUP:128]))
        state = state * total + jnp.concatenate(pieces, 1)
        decay = decay * total
        offset = offset + log_total
    return state, decay, offset


def local_kernel(where_ref, sums, reward, entering, offsets, recept, pair, decay, local, queries, *, first, count, first_token):
    start = where_ref[1]
    channels = local.shape[1]
    line = lax.broadcasted_iota(jnp.int32, (SUB, 1), 0)
    lane = lax.broadcasted_iota(jnp.int32, (SUB, 128), 1)
    two_t = lax.broadcasted_iota(jnp.int32, (2 * SUB, SUB), 0) % SUB
    two_s = lax.broadcasted_iota(jnp.int32, (2 * SUB, SUB), 1)

    def apart(a):
        zero = jnp.zeros_like(a)
        first = lane[0 : a.shape[0]] < GROUP
        return jnp.concatenate([jnp.where(first, a, zero), jnp.where(first, zero, a)], 0)

    def spread(part, half):
        rows = []
        for at in range(0, SUB, half):
            rows += [part[at : at + half]] * 2
        return jnp.concatenate(rows, 0)

    row = lax.broadcasted_iota(jnp.int32, (128, 128), 0)
    col = lax.broadcasted_iota(jnp.int32, (128, 128), 1)
    ones = jnp.where((row // GROUP) == (col // GROUP), 1.0, 0.0).astype(BF16)

    for n in range(count):
        c = first + n
        at = SUB * c - first_token
        there = slice(at, at + SUB)
        r = recept[there, :]
        k, v_wide = [pair[there, channels * i : channels * i + channels] for i in range(2)]
        w = decay[there, :]
        v = v_wide.astype(BF16)
        w = jnp.maximum(w, FLOOR)
        sides, rights = [], []
        exponents = dot(sums[0 : 7 * SUB, :], split_two(w))
        for level, half in enumerate(HALVES):
            right = (line // half) % 2 == 1
            side = jnp.where(right, r, k) * jnp.exp(exponents[SUB * level : SUB * level + SUB, :])
            sides.append(side.astype(BF16))
            if half >= 8:
                tops = [side[top : top + half] for top in range(half, SUB, 2 * half)]
                rights.append(jnp.concatenate(tops, 0).astype(BF16))
        before_here = exponents[6 * SUB : 7 * SUB, :]
        late = (line + c * SUB) >= start
        begins_late = (c * SUB - 1) >= start if c else jnp.bool_(False)
        reach = jnp.where(late == begins_late, r * jnp.exp(before_here), 0.0).astype(BF16)
        offset = offsets[c : c + 1, :]
        rows = slice(SUB * n, SUB * n + SUB)
        queries[rows, :] = jnp.where(late, 0.0, r * jnp.exp(offset + before_here)).astype(BF16)
        own = (r * reward[...] * k).astype(BF16)
        same = ((two_t + c * SUB) >= start) == ((two_s + c * SUB) >= start)
        for p in range(channels // 128):
            cols = slice(128 * p, 128 * p + 128)
            scores = jnp.zeros((2 * SUB, SUB), F32)
            for level, half in enumerate(HALVES):
                side = sides[level][:, cols]
                if half >= 8:
                    part = spread(dot_nt(apart(rights[level][:, cols]), side), half)
                else:
                    part = dot_nt(apart(side), side)
                here = (two_t // (2 * half) == two_s // (2 * half)) & ((two_t // half) % 2 == 1) & ((two_s // half) % 2 == 0)
                scores = jnp.where(here, part, scores)
            both = dot(jnp.where(same, scores, 0.0).astype(BF16), v[:, cols])
            out = jnp.where(lane < GROUP, both[0:SUB], both[SUB : 2 * SUB])
            out = out + dot(own[:, cols], ones) * v_wide[:, cols]
            local[rows, cols] = out + dot_nt(reach[:, cols], apart(entering[c, :, cols]))


def local_outputs(where, sums, reward, entering, offsets, recept, pair, decay, numbers, first_token):
    channels = entering.shape[2]
    tokens = len(numbers) * SUB
    return pl.pallas_call(
        functools.partial(local_kernel, first=numbers[0], count=len(numbers), first_token=first_token),
        in_specs=[SMEM] + [VMEM] * 7,
        out_specs=[VMEM] * 2,
        out_shape=[pltpu.VMEM((tokens, channels), F32), pltpu.VMEM((tokens, channels), BF16)],
        compiler_params=pltpu.CompilerParams(vmem_limit_bytes=8 * 1024 * 1024),
        cost_estimate=pl.CostEstimate(flops=2 * 10**9, bytes_accessed=3 * 10**6, transcendentals=0),
    )(where, *map(in_vmem, (sums, reward, entering, offsets, recept, pair, decay)))


def unpack(ref):
    return ref[SUB : SUB + 1].astype(F32) + ref[SUB + 1 : SUB + 2].astype(F32), ref[0:SUB].astype(F32)


def pack(ref, decay, state):
    high = decay.astype(BF16)
    low = (decay - high.astype(F32)).astype(BF16)
    wide = (8, decay.shape[1])
    line = lax.broadcasted_iota(jnp.int32, wide, 0)
    high, low = high.astype(F32), low.astype(F32)
    ref[0:SUB, :] = state.astype(BF16)
    ref[SUB : SUB + 8, :] = jnp.where(line == 0, high, jnp.where(line == 1, low, 0.0)).astype(BF16)


def store(ref, decay, state):
    ref[0:SUB, :] = state
    ref[SUB : SUB + 8, :] = jnp.broadcast_to(decay, (8, decay.shape[1]))


def combine(earlier, later):
    return earlier[0] * later[0], later[0] * earlier[1] + later[1]


def choose(flag, a, b):
    return tuple(jnp.where(flag, u, v) for u, v in zip(a, b))


def along_axis(here, own, received, before):
    pieces = [own] + [unpack(ref) for ref in received]
    length = len(pieces)
    start = (jnp.ones_like(own[0]), jnp.zeros_like(own[1]))
    inside, so_far = start, None
    for m in range(length):
        from_m = pieces[m]
        for other in range(1, length):
            from_m = choose(here == other, pieces[m ^ other], from_m)
        if m:
            inside = choose(here == m, so_far, inside)
        so_far = from_m if so_far is None else combine(so_far, from_m)
    return inside if before is None else combine(inside, before), so_far


def merge_kernel(where_ref, *refs, place, count, opening):
    whole, refs = refs[0], refs[1:]
    before = None
    if not opening:
        before, refs = (refs[0][SUB : SUB + 1], refs[0][0:SUB]), refs[1:]
    received, (whole_out, packed_out, before_out) = refs[:count], refs[count:]
    own = (whole[SUB : SUB + 1], whole[0:SUB])
    before, total = along_axis(where_ref[place], own, received, before)
    store(whole_out, *total)
    pack(packed_out, *total)
    store(before_out, *before)


def merge(where, place, whole, before, received):
    channels = whole.shape[1]
    operands = [whole] + ([] if before is None else [before]) + received
    return pl.pallas_call(
        functools.partial(merge_kernel, place=place, count=len(received), opening=before is None),
        in_specs=[SMEM] + [VMEM] * len(operands),
        out_specs=[VMEM] * 3,
        out_shape=[
            jax.ShapeDtypeStruct((SUB + 8, channels), F32),
            jax.ShapeDtypeStruct((SUB + 8, channels), BF16),
            jax.ShapeDtypeStruct((SUB + 8, channels), F32),
        ],
        compiler_params=pltpu.CompilerParams(vmem_limit_bytes=4 * 1024 * 1024),
        cost_estimate=pl.CostEstimate(flops=10**8, bytes_accessed=10**6, transcendentals=0),
    )(where, *operands)


def finish_kernel(where_ref, *refs, parts, place):
    locals_, queries, refs = refs[:parts], refs[parts : 2 * parts], refs[2 * parts :]
    gain, shift, whole, before, *received, out, held, ready = refs
    own = (whole[SUB : SUB + 1], whole[0:SUB])
    (_, incoming), _ = along_axis(where_ref[place], own, received, (before[SUB : SUB + 1], before[0:SUB]))
    incoming = incoming.astype(BF16)
    channels = gain.shape[1]
    wide = 256
    lane = lax.broadcasted_iota(jnp.int32, (SUB, wide), 1) // GROUP
    row = lax.broadcasted_iota(jnp.int32, (wide, wide), 0)
    col = lax.broadcasted_iota(jnp.int32, (wide, wide), 1)
    average = jnp.where((row // GROUP) == (col // GROUP), 1.0 / GROUP, 0.0).astype(BF16)
    blocks = []
    for p in range(channels // wide):
        st = incoming[:, wide * p : wide * p + wide]
        blocks.append(jnp.concatenate([jnp.where(lane == h, st, jnp.zeros_like(st)) for h in range(wide // GROUP)], 0))
    copies = []
    at = 0
    for i in range(parts):
        rows = slice(at, at + locals_[i].shape[0])
        at = rows.stop
        for p in range(channels // wide):
            cols = slice(wide * p, wide * p + wide)
            o = locals_[i][:, cols] + dot_nt(queries[i][:, cols], blocks[p])
            centred = o - dot(o.astype(BF16), average)
            variance = dot((centred * centred).astype(BF16), average)
            normed = centred * lax.rsqrt(variance + 0.00064)
            held[rows, cols] = (normed * gain[:, cols] + shift[:, cols]).astype(BF16)
        copies.append(pltpu.make_async_copy(held.at[rows, :], out.at[rows, :], ready.at[i]))
        copies[-1].start()
    for copy in copies:
        copy.wait()


def finish(where, place, locals_, queries, gain, shift, whole, before, received):
    parts = len(locals_)
    tokens, channels = sum(a.shape[0] for a in locals_), gain.shape[1]
    return pl.pallas_call(
        functools.partial(finish_kernel, parts=parts, place=place),
        in_specs=[SMEM] + [VMEM] * (2 * parts + 4 + len(received)),
        out_specs=pl.BlockSpec(memory_space=pltpu.HBM),
        scratch_shapes=[pltpu.VMEM((tokens, channels), BF16), pltpu.SemaphoreType.DMA((parts,))],
        out_shape=jax.ShapeDtypeStruct((tokens, channels), BF16),
        compiler_params=pltpu.CompilerParams(vmem_limit_bytes=8 * 1024 * 1024),
        cost_estimate=pl.CostEstimate(flops=10**9, bytes_accessed=2 * 10**6, transcendentals=0),
    )(where, *map(in_vmem, (*locals_, *queries, gain, shift)), whole, before, *received)


def inner(
    layer_inputs,
    article_opening,
    blending_ratios,
    blending_narrow_operand,
    blending_widen_operand,
    fading_narrow_operand,
    fading_widen_operand,
    fading_anchor,
    immediate_reward,
    acceptance_weights,
    lookup_weights,
    payload_weights,
    group_scaling_weight,
    group_scaling_shift,
):
    x = layer_inputs
    places = [lax.axis_index(axis).astype(jnp.int32) for axis in (MP, *SEQ)]
    where = jnp.stack([places[0], article_opening[0], *places[1:]])
    shards = lax.axis_size(SEQ)

    def across_far(a):
        return lax.ppermute(a, ("y_hi", "y_lo"), [(i, i ^ 3) for i in range(4)])

    def partner(a):
        return xor_permute(a, MP, 1)

    def across(a):
        return xor_permute(a, MP, 2)

    late_a, late_b, own_early, last = cut(where, x)
    own_late = [late_a, late_b]
    far_late_a = across(late_a)
    far_narrow = across_far(blending_narrow_operand)
    near_narrow = partner(blending_narrow_operand)
    far_fading = across_far(fading_narrow_operand)
    near_fading = partner(fading_narrow_operand)
    near_late_a = partner(late_a)
    before = lax.ppermute(last, SEQ, [(i, i + 1) for i in range(shards - 1)])
    far_late_b = across(late_b)
    near_late_b = partner(late_b)
    own_early = lax.dynamic_update_slice(own_early, before, (0, 0))
    far_early = across(own_early)
    near_early = partner(own_early)
    sums = jnp.asarray(sum_rows(), BF16)
    widen, ratios, narrow, fade_widen, anchor, sums, reward, gain, shift, fading = load(
        where, ("lanes", blending_widen_operand), ("plain", blending_ratios),
        ("plain", blending_narrow_operand), ("plain", fading_widen_operand), ("plain", fading_anchor[None]),
        ("plain", sums), ("plain", immediate_reward[None]), ("plain", group_scaling_weight[None]),
        ("plain", group_scaling_shift[None]), ("plain", fading_narrow_operand),
    )
    next_late_a = partner(far_late_a)
    next_narrow = partner(far_narrow)
    next_fading = partner(far_fading)
    next_late_b = partner(far_late_b)
    narrows = [narrow, near_narrow, far_narrow, next_narrow]
    fadings = [fading, near_fading, far_fading, next_fading]
    pieces = [own_late, [near_late_a, near_late_b], [far_late_a, far_late_b], [next_late_a, next_late_b]]
    late, late_recept, fading_rows, w_k, w_v, w_r = project_late(
        where, pieces, narrows, ratios, widen, lookup_weights, payload_weights, acceptance_weights
    )
    far_early, late = lax.optimization_barrier((far_early, late))
    late_decay, partial, reach, late_whole = decay_late(where, fading_rows, fadings, fade_widen, anchor, sums, late)
    next_early = partner(far_early)
    pieces = [[own_early], [near_early], [far_early], [next_early]]
    early, decay, entering, offsets, whole, packed, diffs, hidden = project_early(
        where, pieces, narrows, fadings, (ratios, widen, w_k, w_v), fade_widen, anchor, sums,
        partial, reach, late_whole,
    )
    early_recept = recept_early(where, pieces, diffs, hidden, ratios, widen, w_r)
    middle, end = LAST // SUB, x.shape[0] // SUB
    jobs = (
        (early_recept, early, decay, tuple(range(middle)), 0),
        (late_recept, late, late_decay, tuple(range(middle, middle + 1)), LAST),
        (late_recept, late, late_decay, tuple(range(middle + 1, end)), LAST),
    )
    outputs = []
    for job in jobs:
        outputs.append(local_outputs(where, sums, reward, entering, offsets, *job))
    before = None
    for axis in reversed(SEQ):
        received = []
        for k in range(1, lax.axis_size(axis)):
            received.append(xor_permute(packed, axis, k))
        place = 2 + SEQ.index(axis)
        if axis != SEQ[0]:
            whole, packed, before = merge(where, place, whole, before, received)
    locals_, queries = zip(*outputs)
    return finish(where, place, locals_, queries, gain, shift, whole, before, received)


def solution(mesh):
    torus = Mesh(mesh.devices.reshape(4, 4, 2, 2, 2), ("z", "x", "y_hi", "y_lo", "core"))
    placed = (
        P(SEQ, MP),
        P(SEQ),
        P(),
        P(MP, None),
        P(),
        P(MP, None),
        P(None, MP),
        P(MP),
        P(MP),
        P(None, MP),
        P(None, MP),
        P(None, MP),
        P(MP),
        P(MP),
    )
    return jax.shard_map(inner, mesh=torus, in_specs=placed, out_specs=P(SEQ, MP), check_vma=False)
```

```python
import functools

import jax
import jax.numpy as jnp
import numpy as np
from jax import lax
from jax.experimental import pallas as pl
from jax.experimental.pallas import tpu as pltpu
from jax.sharding import Mesh
from jax.sharding import PartitionSpec as P


F32 = jnp.float32
BF16 = jnp.bfloat16
GROUP = 64
SUB = 64
LAST = 256
SPLIT = 128
CTX = 16
HALVES = (32, 16, 8, 4, 2, 1)
FLOOR = -100.0
SEQ = ("z", "x", "y_hi")
MP = ("y_lo", "core")


def xor_permute(array, axes, flip):
    length = lax.axis_size(axes)
    return lax.ppermute(array, axes, [(i, i ^ flip) for i in range(length)])


def dot(a, b):
    return jnp.dot(a, b, preferred_element_type=F32)


def dot_nt(a, b):
    return lax.dot_general(a, b, (((1,), (1,)), ((), ())), preferred_element_type=F32)


def dot_tn(a, b):
    return lax.dot_general(a, b, (((0,), (0,)), ((), ())), preferred_element_type=F32)


def sum_rows():
    t = np.arange(SUB)[:, None]
    j = np.arange(SUB)[None, :]
    blocks = []
    for half in HALVES:
        middle = (t // (2 * half)) * (2 * half) + half - 1
        right = t > middle
        blocks.append(np.where(right, (j > middle) & (j < t), (j > t) & (j <= middle)))
    blocks.append(j < t)
    blocks.append(j > t)
    one = np.concatenate(blocks, 0)
    return np.concatenate([one, one], 1).astype(np.float32)


SMEM = pl.BlockSpec(memory_space=pltpu.SMEM)
VMEM = pl.BlockSpec(memory_space=pltpu.VMEM)


def in_hbm(array):
    return pltpu.with_memory_space_constraint(array, pltpu.HBM)


def in_vmem(array):
    return pltpu.with_memory_space_constraint(array, pltpu.VMEM)


def cut_kernel(where_ref, x, late_a, late_b, early, last, ready):
    tokens = x.shape[0]
    moves = (
        (x.at[LAST - CTX : LAST + SPLIT, :], late_a),
        (x.at[tokens - CTX :, :], last),
        (x.at[LAST + SPLIT :, :], late_b),
        (x.at[0:LAST, :], early.at[CTX:, :]),
    )
    copies = [pltpu.make_async_copy(a, b, ready.at[i]) for i, (a, b) in enumerate(moves)]
    for copy in copies:
        copy.start()
    early[0:CTX, :] = jnp.zeros((CTX, early.shape[1]), BF16)
    for copy in copies:
        copy.wait()


def cut(where, x):
    tokens, width = x.shape
    return pl.pallas_call(
        cut_kernel,
        in_specs=[SMEM, pl.BlockSpec(memory_space=pltpu.HBM)],
        out_specs=[VMEM] * 4,
        scratch_shapes=[pltpu.SemaphoreType.DMA((4,))],
        out_shape=[
            pltpu.VMEM((CTX + SPLIT, width), BF16),
            pltpu.VMEM((tokens - LAST - SPLIT, width), BF16),
            pltpu.VMEM((CTX + LAST, width), BF16),
            pltpu.VMEM((CTX, width), BF16),
        ],
        compiler_params=pltpu.CompilerParams(vmem_limit_bytes=2**20),
        cost_estimate=pl.CostEstimate(flops=10**6, bytes_accessed=2 * 10**6, transcendentals=0),
    )(where, in_hbm(x))


def load_kernel(where_ref, *refs, kinds):
    count = len(kinds)
    ready = refs[2 * count]
    copies = []
    for i, kind in enumerate(kinds):
        source, target = refs[i], refs[count + i]
        if kind == "plain":
            copies.append(pltpu.make_async_copy(source, target, ready.at[i, 0]))
            continue
        width = target.shape[-1] if kind == "lanes" else target.shape[1]
        for j in range(4):
            there = pl.ds(pl.multiple_of((where_ref[0] ^ j) * width, width), width)
            block = source.at[:, :, there] if kind == "lanes" else source.at[there, :]
            copies.append(pltpu.make_async_copy(block, target.at[j], ready.at[i, j]))
    for copy in copies:
        copy.start()
    for copy in copies:
        copy.wait()


def load(where, *jobs):
    kinds, arrays = zip(*jobs)
    shapes = []
    for kind, a in jobs:
        if kind == "rows":
            shapes.append((4, a.shape[0] // 4, a.shape[1]))
        elif kind == "lanes":
            shapes.append((4, *a.shape[:2], a.shape[2] // 4))
        else:
            shapes.append(a.shape)
    return pl.pallas_call(
        functools.partial(load_kernel, kinds=kinds),
        in_specs=[SMEM] + [pl.BlockSpec(memory_space=pltpu.HBM)] * len(jobs),
        out_specs=[VMEM] * len(jobs),
        scratch_shapes=[pltpu.SemaphoreType.DMA((len(jobs), 4))],
        out_shape=[pltpu.VMEM(shape, a.dtype) for shape, a in zip(shapes, arrays)],
        compiler_params=pltpu.CompilerParams(vmem_limit_bytes=2**20),
        cost_estimate=pl.CostEstimate(flops=3 * 10**9, bytes_accessed=8 * 10**6, transcendentals=0),
    )(where, *map(in_hbm, arrays))


def read_rows(refs, cols):
    parts = [ref[:, cols] for ref in refs]
    return parts[0] if len(parts) == 1 else jnp.concatenate(parts, 0)


def mix_rows(me, start, first_token, pieces, narrows, weights, diffs, slots, consume, branches=(0, 1, 2, 3), ranked=None):
    ratios, widen = weights
    tokens, width = diffs.shape[1:]
    tile = 256
    line = lax.broadcasted_iota(jnp.int32, (tokens, tile), 0)
    first = lax.broadcasted_iota(jnp.int32, (8, tile), 0) == 0
    opens = line + first_token == start

    rank = jnp.zeros((tokens, 256), F32)
    for j in range(4):
        base = (me ^ j) * width
        parts = []
        for n in range(width // tile):
            cols = slice(tile * n, tile * n + tile)
            rows = read_rows(pieces[j], cols).astype(F32)
            x = rows[CTX:]
            before = pltpu.roll(x, 1, 0)
            before = jnp.concatenate([jnp.where(first, rows[CTX - 1 : CTX], before[0:8]), before[8:]], 0)
            d = jnp.where(opens, 0.0, before) - x
            diffs[j, :, cols] = d
            ratio = ratios[0:1, pl.ds(pl.multiple_of(base + tile * n, tile), tile)]
            parts.append((x + d * ratio).astype(BF16))
        rank = rank + dot(jnp.concatenate(parts, 1), narrows[j][...])
    if ranked:
        ranked()
    total = jnp.tanh(rank).astype(BF16)
    hidden = [total[:, 64 * b : 64 * b + 64] for b in range(4)]

    def mix(j):
        base = (me ^ j) * width
        for n in range(width // tile):
            cols = slice(tile * n, tile * n + tile)
            there = pl.ds(pl.multiple_of(base + tile * n, tile), tile)
            x = read_rows(pieces[j], cols)[CTX:].astype(F32)
            d = diffs[j, :, cols]
            for b in branches:
                delta = dot(hidden[b], widen[j, b, :, cols])
                slots(j, b)[:, cols] = (x + d * (ratios[b + 1 : b + 2, there] + delta)).astype(BF16)

    mix(0)
    for j in range(4):
        if j < 3:
            mix(j + 1)
        consume(j)
    return hidden


def add_product(out, cols, j, rows, weights):
    part = dot(rows[...], weights[j])
    if j == 0:
        out[:, cols] = part
    else:
        out[:, cols] += part


def decay_of(low, fade_widen, anchor):
    return -jnp.exp(anchor[...] + dot(jnp.tanh(low).astype(BF16), fade_widen[...]))


def take_pieces(refs, counts):
    pieces = []
    for count in counts:
        pieces.append(refs[:count])
        refs = refs[count:]
    return pieces, refs


def late_kernel(where_ref, *refs, counts):
    pieces, refs = take_pieces(refs, counts)
    narrows, refs = refs[0:4], refs[4:]
    ratios, widen, w_k_far, w_v_far, w_r_far, pair, recept, fading_rows, w_k, w_v, w_r, diffs, mixed, ready = refs
    channels, width = recept.shape[1], w_k.shape[1]

    def fetch(j, i):
        there = pl.ds(pl.multiple_of((where_ref[0] ^ j) * width, width), width)
        source, target = ((w_k_far, w_k), (w_v_far, w_v), (w_r_far, w_r))[i]
        return pltpu.make_async_copy(source.at[there, :], target.at[j], ready.at[j, i])

    def start_fetches(j):
        for i in range(3):
            fetch(j, i).start()

    start_fetches(0)
    start_fetches(1)

    def slots(j, b):
        return fading_rows.at[j] if b == 0 else mixed.at[j % 2, b - 1]

    def consume(j):
        fetch(j, 0).wait()
        add_product(pair, slice(0, channels), j, slots(j, 1), w_k)
        fetch(j, 1).wait()
        add_product(pair, slice(channels, 2 * channels), j, slots(j, 2), w_v)
        fetch(j, 2).wait()
        add_product(recept, slice(None), j, slots(j, 3), w_r)

    def ranked():
        start_fetches(2)
        start_fetches(3)

    mix_rows(where_ref[0], where_ref[1], LAST, pieces, narrows, (ratios, widen), diffs, slots, consume, ranked=ranked)


def decay_kernel(where_ref, rows, *refs):
    fadings, (fade_widen, anchor, sums, pair, out, partial, reach, whole) = refs[0:4], refs[4:]
    tokens, _ = out.shape
    low = dot(rows[0], fadings[0][...])
    for j in range(1, 4):
        low = low + dot(rows[j], fadings[j][...])
    out[...] = decay_of(low, fade_widen, anchor)
    count = tokens // SUB

    def note(n, state, decay, offset):
        partial[n] = state
        reach[n : n + 1, :] = decay
        reach[count + n : count + n + 1, :] = offset

    numbers = range(LAST // SUB, LAST // SUB + count)
    state, decay, _ = add_states(where_ref[1], sums, pair, out, numbers, LAST, note)
    store(whole, decay, state)


def early_kernel(where_ref, *refs, counts):
    pieces, refs = take_pieces(refs, counts)
    narrows, fadings, refs = refs[0:4], refs[4:8], refs[8:]
    ratios, widen, w_k, w_v, fade_widen, anchor, sums, partial, reach, late_whole = refs[:10]
    pair, decay, entering, offsets, whole, packed, diffs, hidden, mixed = refs[10:]
    channels = decay.shape[1]
    low = [None]

    def slots(j, b):
        return mixed.at[j % 2, b]

    def consume(j):
        part = dot(slots(j, 0)[...], fadings[j][...])
        low[0] = part if j == 0 else low[0] + part
        add_product(pair, slice(0, channels), j, slots(j, 1), w_k)
        add_product(pair, slice(channels, 2 * channels), j, slots(j, 2), w_v)

    ranks = mix_rows(
        where_ref[0], where_ref[1], 0, pieces, narrows, (ratios, widen), diffs, slots, consume, branches=(0, 1, 2)
    )
    hidden[...] = ranks[3]
    decay[...] = decay_of(low[0], fade_widen, anchor)

    def note(n, state, _, offset):
        entering[n] = state.astype(BF16)
        offsets[n : n + 1, :] = offset

    count, more = LAST // SUB, partial.shape[0]
    state, total, offset = add_states(where_ref[1], sums, pair, decay, range(count), 0, note)
    final = combine((total, state), (late_whole[SUB : SUB + 1], late_whole[0:SUB]))
    store(whole, *final)
    pack(packed, *final)
    for n in range(more):
        entering[count + n] = (partial[n] + reach[n : n + 1, :] * state).astype(BF16)
        offsets[count + n : count + n + 1, :] = offset + reach[more + n : more + n + 1, :]


def recept_kernel(where_ref, *refs, counts):
    pieces, refs = take_pieces(refs, counts)
    diffs, hidden, ratios, widen, w_r, out, mixed = refs
    width = diffs.shape[2]
    tile = 256
    for j in range(4):
        base = (where_ref[0] ^ j) * width
        for n in range(width // tile):
            cols = slice(tile * n, tile * n + tile)
            there = pl.ds(pl.multiple_of(base + tile * n, tile), tile)
            x = read_rows(pieces[j], cols)[CTX:].astype(F32)
            delta = dot(hidden[...], widen[j, 3, :, cols])
            mixed[j, :, cols] = (x + diffs[j, :, cols] * (ratios[4:5, there] + delta)).astype(BF16)
        add_product(out, slice(None), j, mixed.at[j], w_r)


def recept_early(where, pieces, diffs, hidden, ratios, widen, w_r):
    tokens, width = diffs.shape[1:]
    counts = tuple(len(p) for p in pieces)
    operands = [a for p in pieces for a in p]
    return pl.pallas_call(
        functools.partial(recept_kernel, counts=counts),
        in_specs=[SMEM] + [VMEM] * (len(operands) + 5),
        out_specs=VMEM,
        scratch_shapes=[pltpu.VMEM((4, tokens, width), BF16)],
        out_shape=pltpu.VMEM((tokens, w_r.shape[2]), F32),
        compiler_params=pltpu.CompilerParams(vmem_limit_bytes=7 * 2**20),
        cost_estimate=pl.CostEstimate(flops=2 * 10**9, bytes_accessed=5 * 10**6, transcendentals=0),
    )(where, *operands, *map(in_vmem, (diffs, hidden, ratios, widen, w_r)))


def project_late(where, pieces, narrows, ratios, widen, w_k, w_v, w_r):
    width, channels = w_k.shape[0] // 4, w_k.shape[1]
    counts = tuple(len(p) for p in pieces)
    tokens = sum(a.shape[0] for a in pieces[0]) - CTX
    operands = [a for p in pieces for a in p] + narrows
    return pl.pallas_call(
        functools.partial(late_kernel, counts=counts),
        in_specs=[SMEM] + [VMEM] * (len(operands) + 2) + [pl.BlockSpec(memory_space=pltpu.HBM)] * 3,
        out_specs=[VMEM] * 6,
        scratch_shapes=[
            pltpu.VMEM((4, tokens, width), F32),
            pltpu.VMEM((2, 3, tokens, width), BF16),
            pltpu.SemaphoreType.DMA((4, 3)),
        ],
        out_shape=[
            pltpu.VMEM((tokens, 2 * channels), F32),
            pltpu.VMEM((tokens, channels), F32),
            pltpu.VMEM((4, tokens, width), BF16),
            pltpu.VMEM((4, width, channels), BF16),
            pltpu.VMEM((4, width, channels), BF16),
            pltpu.VMEM((4, width, channels), BF16),
        ],
        compiler_params=pltpu.CompilerParams(vmem_limit_bytes=(4 * 1024 + 40 * tokens) * 1024),
        cost_estimate=pl.CostEstimate(flops=25 * 10**6 * tokens, bytes_accessed=17 * 10**6, transcendentals=0),
    )(where, *operands, *map(in_vmem, (ratios, widen)), *map(in_hbm, (w_k, w_v, w_r)))


def decay_late(where, rows, fadings, fade_widen, anchor, sums, pair):
    tokens, channels = rows.shape[1], anchor.shape[1]
    count = tokens // SUB
    return pl.pallas_call(
        decay_kernel,
        in_specs=[SMEM] + [VMEM] * 9,
        out_specs=[VMEM] * 4,
        out_shape=[
            pltpu.VMEM((tokens, channels), F32),
            pltpu.VMEM((count, SUB, channels), F32),
            pltpu.VMEM((2 * count, channels), F32),
            pltpu.VMEM((SUB + 8, channels), F32),
        ],
        compiler_params=pltpu.CompilerParams(vmem_limit_bytes=5 * 2**20),
        cost_estimate=pl.CostEstimate(flops=10**9, bytes_accessed=2 * 10**6, transcendentals=0),
    )(where, in_vmem(rows), *fadings, *map(in_vmem, (fade_widen, anchor, sums, pair)))


def project_early(where, pieces, narrows, fadings, weights, *rest):
    width, channels = weights[2].shape[1:]
    counts = tuple(len(p) for p in pieces)
    operands = [a for p in pieces for a in p] + narrows + fadings
    return pl.pallas_call(
        functools.partial(early_kernel, counts=counts),
        in_specs=[SMEM] + [VMEM] * (len(operands) + len(weights) + len(rest)),
        out_specs=[VMEM] * 8,
        scratch_shapes=[pltpu.VMEM((2, 3, LAST, width), BF16)],
        out_shape=[
            pltpu.VMEM((LAST, 2 * channels), F32),
            pltpu.VMEM((LAST, channels), F32),
            pltpu.VMEM((8, SUB, channels), BF16),
            pltpu.VMEM((8, channels), F32),
            jax.ShapeDtypeStruct((SUB + 8, channels), F32),
            jax.ShapeDtypeStruct((SUB + 8, channels), BF16),
            pltpu.VMEM((4, LAST, width), F32),
            pltpu.VMEM((LAST, 64), BF16),
        ],
        compiler_params=pltpu.CompilerParams(vmem_limit_bytes=(5 * 1024 + 16 * LAST) * 1024),
        cost_estimate=pl.CostEstimate(flops=25 * 10**6 * LAST, bytes_accessed=17 * 10**6, transcendentals=0),
    )(where, *operands, *map(in_vmem, (*weights, *rest)))


def split_two(w):
    high = w.astype(BF16)
    low = (w - high.astype(F32)).astype(BF16)
    return jnp.concatenate([high, low], 0)


def add_states(start, sums, pair, decays, numbers, first_token, note):
    channels = decays.shape[1]
    line = lax.broadcasted_iota(jnp.int32, (SUB, 1), 0)
    lane = lax.broadcasted_iota(jnp.int32, (SUB, 128), 1)
    state = jnp.zeros((SUB, channels), F32)
    decay = jnp.ones((1, channels), F32)
    offset = jnp.zeros((1, channels), F32)
    for n, c in enumerate(numbers):
        note(n, state, decay, offset)
        at = SUB * c - first_token
        w = jnp.maximum(decays[at : at + SUB, :], FLOOR)
        k = pair[at : at + SUB, 0:channels]
        v = pair[at : at + SUB, channels : 2 * channels].astype(BF16)
        tail = dot(sums[7 * SUB : 8 * SUB, :], split_two(w))
        ends_late = (c * SUB + SUB - 1) >= start
        begins_late = (c * SUB - 1) >= start if c else jnp.bool_(False)
        late = (line + c * SUB) >= start
        log_total = tail[0:1, :] + w[0:1, :]
        total = jnp.where(begins_late == ends_late, jnp.exp(log_total), 0.0)
        kk = jnp.where(late == ends_late, k * jnp.exp(tail), 0.0).astype(BF16)
        pieces = []
        for p in range(channels // 128):
            cols = slice(128 * p, 128 * p + 128)
            both = dot_tn(v[:, cols], kk[:, cols])
            pieces.append(jnp.where(lane < GROUP, both[0:GROUP], both[GROUP:128]))
        state = state * total + jnp.concatenate(pieces, 1)
        decay = decay * total
        offset = offset + log_total
    return state, decay, offset


def local_kernel(where_ref, sums, reward, entering, offsets, recept, pair, decay, local, queries, *, first, count, first_token):
    start = where_ref[1]
    channels = local.shape[1]
    line = lax.broadcasted_iota(jnp.int32, (SUB, 1), 0)
    lane = lax.broadcasted_iota(jnp.int32, (SUB, 128), 1)
    two_t = lax.broadcasted_iota(jnp.int32, (2 * SUB, SUB), 0) % SUB
    two_s = lax.broadcasted_iota(jnp.int32, (2 * SUB, SUB), 1)

    def apart(a):
        zero = jnp.zeros_like(a)
        first = lane[0 : a.shape[0]] < GROUP
        return jnp.concatenate([jnp.where(first, a, zero), jnp.where(first, zero, a)], 0)

    def spread(part, half):
        rows = []
        for at in range(0, SUB, half):
            rows += [part[at : at + half]] * 2
        return jnp.concatenate(rows, 0)

    row = lax.broadcasted_iota(jnp.int32, (128, 128), 0)
    col = lax.broadcasted_iota(jnp.int32, (128, 128), 1)
    ones = jnp.where((row // GROUP) == (col // GROUP), 1.0, 0.0).astype(BF16)

    for n in range(count):
        c = first + n
        at = SUB * c - first_token
        there = slice(at, at + SUB)
        r = recept[there, :]
        k, v_wide = [pair[there, channels * i : channels * i + channels] for i in range(2)]
        w = decay[there, :]
        v = v_wide.astype(BF16)
        w = jnp.maximum(w, FLOOR)
        sides, rights = [], []
        exponents = dot(sums[0 : 7 * SUB, :], split_two(w))
        for level, half in enumerate(HALVES):
            right = (line // half) % 2 == 1
            side = jnp.where(right, r, k) * jnp.exp(exponents[SUB * level : SUB * level + SUB, :])
            sides.append(side.astype(BF16))
            if half >= 8:
                tops = [side[top : top + half] for top in range(half, SUB, 2 * half)]
                rights.append(jnp.concatenate(tops, 0).astype(BF16))
        before_here = exponents[6 * SUB : 7 * SUB, :]
        late = (line + c * SUB) >= start
        begins_late = (c * SUB - 1) >= start if c else jnp.bool_(False)
        reach = jnp.where(late == begins_late, r * jnp.exp(before_here), 0.0).astype(BF16)
        offset = offsets[c : c + 1, :]
        rows = slice(SUB * n, SUB * n + SUB)
        queries[rows, :] = jnp.where(late, 0.0, r * jnp.exp(offset + before_here)).astype(BF16)
        own = (r * reward[...] * k).astype(BF16)
        same = ((two_t + c * SUB) >= start) == ((two_s + c * SUB) >= start)
        for p in range(channels // 128):
            cols = slice(128 * p, 128 * p + 128)
            scores = jnp.zeros((2 * SUB, SUB), F32)
            for level, half in enumerate(HALVES):
                side = sides[level][:, cols]
                if half >= 8:
                    part = spread(dot_nt(apart(rights[level][:, cols]), side), half)
                else:
                    part = dot_nt(apart(side), side)
                here = (two_t // (2 * half) == two_s // (2 * half)) & ((two_t // half) % 2 == 1) & ((two_s // half) % 2 == 0)
                scores = jnp.where(here, part, scores)
            both = dot(jnp.where(same, scores, 0.0).astype(BF16), v[:, cols])
            out = jnp.where(lane < GROUP, both[0:SUB], both[SUB : 2 * SUB])
            out = out + dot(own[:, cols], ones) * v_wide[:, cols]
            local[rows, cols] = out + dot_nt(reach[:, cols], apart(entering[c, :, cols]))


def local_outputs(where, sums, reward, entering, offsets, recept, pair, decay, numbers, first_token):
    channels = entering.shape[2]
    tokens = len(numbers) * SUB
    return pl.pallas_call(
        functools.partial(local_kernel, first=numbers[0], count=len(numbers), first_token=first_token),
        in_specs=[SMEM] + [VMEM] * 7,
        out_specs=[VMEM] * 2,
        out_shape=[pltpu.VMEM((tokens, channels), F32), pltpu.VMEM((tokens, channels), BF16)],
        compiler_params=pltpu.CompilerParams(vmem_limit_bytes=8 * 1024 * 1024),
        cost_estimate=pl.CostEstimate(flops=2 * 10**9, bytes_accessed=3 * 10**6, transcendentals=0),
    )(where, *map(in_vmem, (sums, reward, entering, offsets, recept, pair, decay)))


def unpack(ref):
    return ref[SUB : SUB + 1].astype(F32) + ref[SUB + 1 : SUB + 2].astype(F32), ref[0:SUB].astype(F32)


def pack(ref, decay, state):
    high = decay.astype(BF16)
    low = (decay - high.astype(F32)).astype(BF16)
    wide = (8, decay.shape[1])
    line = lax.broadcasted_iota(jnp.int32, wide, 0)
    high, low = high.astype(F32), low.astype(F32)
    ref[0:SUB, :] = state.astype(BF16)
    ref[SUB : SUB + 8, :] = jnp.where(line == 0, high, jnp.where(line == 1, low, 0.0)).astype(BF16)


def store(ref, decay, state):
    ref[0:SUB, :] = state
    ref[SUB : SUB + 8, :] = jnp.broadcast_to(decay, (8, decay.shape[1]))


def combine(earlier, later):
    return earlier[0] * later[0], later[0] * earlier[1] + later[1]


def choose(flag, a, b):
    return tuple(jnp.where(flag, u, v) for u, v in zip(a, b))


def along_axis(here, own, received, before):
    pieces = [own] + [unpack(ref) for ref in received]
    length = len(pieces)
    start = (jnp.ones_like(own[0]), jnp.zeros_like(own[1]))
    inside, so_far = start, None
    for m in range(length):
        from_m = pieces[m]
        for other in range(1, length):
            from_m = choose(here == other, pieces[m ^ other], from_m)
        if m:
            inside = choose(here == m, so_far, inside)
        so_far = from_m if so_far is None else combine(so_far, from_m)
    return inside if before is None else combine(inside, before), so_far


def merge_kernel(where_ref, *refs, place, count, opening):
    whole, refs = refs[0], refs[1:]
    before = None
    if not opening:
        before, refs = (refs[0][SUB : SUB + 1], refs[0][0:SUB]), refs[1:]
    received, (whole_out, packed_out, before_out) = refs[:count], refs[count:]
    own = (whole[SUB : SUB + 1], whole[0:SUB])
    before, total = along_axis(where_ref[place], own, received, before)
    store(whole_out, *total)
    pack(packed_out, *total)
    store(before_out, *before)


def merge(where, place, whole, before, received):
    channels = whole.shape[1]
    operands = [whole] + ([] if before is None else [before]) + received
    return pl.pallas_call(
        functools.partial(merge_kernel, place=place, count=len(received), opening=before is None),
        in_specs=[SMEM] + [VMEM] * len(operands),
        out_specs=[VMEM] * 3,
        out_shape=[
            jax.ShapeDtypeStruct((SUB + 8, channels), F32),
            jax.ShapeDtypeStruct((SUB + 8, channels), BF16),
            jax.ShapeDtypeStruct((SUB + 8, channels), F32),
        ],
        compiler_params=pltpu.CompilerParams(vmem_limit_bytes=4 * 1024 * 1024),
        cost_estimate=pl.CostEstimate(flops=10**8, bytes_accessed=10**6, transcendentals=0),
    )(where, *operands)


def finish_kernel(where_ref, *refs, parts, place):
    locals_, queries, refs = refs[:parts], refs[parts : 2 * parts], refs[2 * parts :]
    gain, shift, whole, before, *received, out, held, ready = refs
    own = (whole[SUB : SUB + 1], whole[0:SUB])
    (_, incoming), _ = along_axis(where_ref[place], own, received, (before[SUB : SUB + 1], before[0:SUB]))
    incoming = incoming.astype(BF16)
    channels = gain.shape[1]
    wide = 256
    lane = lax.broadcasted_iota(jnp.int32, (SUB, wide), 1) // GROUP
    row = lax.broadcasted_iota(jnp.int32, (wide, wide), 0)
    col = lax.broadcasted_iota(jnp.int32, (wide, wide), 1)
    average = jnp.where((row // GROUP) == (col // GROUP), 1.0 / GROUP, 0.0).astype(BF16)
    blocks = []
    for p in range(channels // wide):
        st = incoming[:, wide * p : wide * p + wide]
        blocks.append(jnp.concatenate([jnp.where(lane == h, st, jnp.zeros_like(st)) for h in range(wide // GROUP)], 0))
    copies = []
    sizes = [a.shape[0] for a in locals_]
    for i in sorted(range(parts), key=lambda i: -sizes[i]):
        rows = slice(sum(sizes[:i]), sum(sizes[: i + 1]))
        for p in range(channels // wide):
            cols = slice(wide * p, wide * p + wide)
            o = locals_[i][:, cols] + dot_nt(queries[i][:, cols], blocks[p])
            centred = o - dot(o.astype(BF16), average)
            variance = dot((centred * centred).astype(BF16), average)
            normed = centred * lax.rsqrt(variance + 0.00064)
            held[rows, cols] = (normed * gain[:, cols] + shift[:, cols]).astype(BF16)
        copies.append(pltpu.make_async_copy(held.at[rows, :], out.at[rows, :], ready.at[i]))
        copies[-1].start()
    for copy in copies:
        copy.wait()


def finish(where, place, locals_, queries, gain, shift, whole, before, received):
    parts = len(locals_)
    tokens, channels = sum(a.shape[0] for a in locals_), gain.shape[1]
    return pl.pallas_call(
        functools.partial(finish_kernel, parts=parts, place=place),
        in_specs=[SMEM] + [VMEM] * (2 * parts + 4 + len(received)),
        out_specs=pl.BlockSpec(memory_space=pltpu.HBM),
        scratch_shapes=[pltpu.VMEM((tokens, channels), BF16), pltpu.SemaphoreType.DMA((parts,))],
        out_shape=jax.ShapeDtypeStruct((tokens, channels), BF16),
        compiler_params=pltpu.CompilerParams(vmem_limit_bytes=8 * 1024 * 1024),
        cost_estimate=pl.CostEstimate(flops=10**9, bytes_accessed=2 * 10**6, transcendentals=0),
    )(where, *map(in_vmem, (*locals_, *queries, gain, shift)), whole, before, *received)


def inner(
    layer_inputs,
    article_opening,
    blending_ratios,
    blending_narrow_operand,
    blending_widen_operand,
    fading_narrow_operand,
    fading_widen_operand,
    fading_anchor,
    immediate_reward,
    acceptance_weights,
    lookup_weights,
    payload_weights,
    group_scaling_weight,
    group_scaling_shift,
):
    x = layer_inputs
    places = [lax.axis_index(axis).astype(jnp.int32) for axis in (MP, *SEQ)]
    where = jnp.stack([places[0], article_opening[0], *places[1:]])
    shards = lax.axis_size(SEQ)

    def across_far(a):
        return lax.ppermute(a, ("y_hi", "y_lo"), [(i, i ^ 3) for i in range(4)])

    def partner(a):
        return xor_permute(a, MP, 1)

    def across(a):
        return xor_permute(a, MP, 2)

    late_a, late_b, own_early, last = cut(where, x)
    own_late = [late_a, late_b]
    far_late_a = across(late_a)
    far_narrow = across_far(blending_narrow_operand)
    near_narrow = partner(blending_narrow_operand)
    far_fading = across_far(fading_narrow_operand)
    near_fading = partner(fading_narrow_operand)
    near_late_a = partner(late_a)
    before = lax.ppermute(last, SEQ, [(i, i + 1) for i in range(shards - 1)])
    far_late_b = across(late_b)
    near_late_b = partner(late_b)
    own_early = lax.dynamic_update_slice(own_early, before, (0, 0))
    far_early = across(own_early)
    near_early = partner(own_early)
    sums = jnp.asarray(sum_rows(), BF16)
    widen, ratios, narrow, fade_widen, anchor, sums, reward, gain, shift, fading = load(
        where, ("lanes", blending_widen_operand), ("plain", blending_ratios),
        ("plain", blending_narrow_operand), ("plain", fading_widen_operand), ("plain", fading_anchor[None]),
        ("plain", sums), ("plain", immediate_reward[None]), ("plain", group_scaling_weight[None]),
        ("plain", group_scaling_shift[None]), ("plain", fading_narrow_operand),
    )
    next_late_a = partner(far_late_a)
    next_narrow = partner(far_narrow)
    next_fading = partner(far_fading)
    next_late_b = partner(far_late_b)
    narrows = [narrow, near_narrow, far_narrow, next_narrow]
    fadings = [fading, near_fading, far_fading, next_fading]
    pieces = [own_late, [near_late_a, near_late_b], [far_late_a, far_late_b], [next_late_a, next_late_b]]
    late, late_recept, fading_rows, w_k, w_v, w_r = project_late(
        where, pieces, narrows, ratios, widen, lookup_weights, payload_weights, acceptance_weights
    )
    far_early, late = lax.optimization_barrier((far_early, late))
    late_decay, partial, reach, late_whole = decay_late(where, fading_rows, fadings, fade_widen, anchor, sums, late)
    next_early = partner(far_early)
    pieces = [[own_early], [near_early], [far_early], [next_early]]
    early, decay, entering, offsets, whole, packed, diffs, hidden = project_early(
        where, pieces, narrows, fadings, (ratios, widen, w_k, w_v), fade_widen, anchor, sums,
        partial, reach, late_whole,
    )
    early_recept = recept_early(where, pieces, diffs, hidden, ratios, widen, w_r)
    middle, end = LAST // SUB, x.shape[0] // SUB
    jobs = (
        (early_recept, early, decay, tuple(range(middle)), 0),
        (late_recept, late, late_decay, tuple(range(middle, middle + 1)), LAST),
        (late_recept, late, late_decay, tuple(range(middle + 1, end)), LAST),
    )
    outputs = []
    for job in jobs:
        outputs.append(local_outputs(where, sums, reward, entering, offsets, *job))
    before = None
    for axis in reversed(SEQ):
        received = []
        for k in range(1, lax.axis_size(axis)):
            received.append(xor_permute(packed, axis, k))
        place = 2 + SEQ.index(axis)
        if axis != SEQ[0]:
            whole, packed, before = merge(where, place, whole, before, received)
    locals_, queries = zip(*outputs)
    return finish(where, place, locals_, queries, gain, shift, whole, before, received)


def solution(mesh):
    torus = Mesh(mesh.devices.reshape(4, 4, 2, 2, 2), ("z", "x", "y_hi", "y_lo", "core"))
    placed = (
        P(SEQ, MP),
        P(SEQ),
        P(),
        P(MP, None),
        P(),
        P(MP, None),
        P(None, MP),
        P(MP),
        P(MP),
        P(None, MP),
        P(None, MP),
        P(None, MP),
        P(MP),
        P(MP),
    )
    return jax.shard_map(inner, mesh=torus, in_specs=placed, out_specs=P(SEQ, MP), check_vma=False)
```
